128 devices in a mesh: time: 16 (over z, y_lo, core), chan: 8 (over y_hi, x).
Axes of the slice: x: 4, y: 4 (y_hi: 2, y_lo: 2; y = y_hi * 2 + y_lo), z: 4, core: 2. Of those that a mesh axis runs over, the one named last changes fastest.
Arguments:
- fade_rate: float32 [1, 8192, 4096], P(None, 'time', 'chan'), may hold values from 0.2 to 2
- update_in: bfloat16 [1, 8192, 4096], P(None, 'time', 'chan'), may hold values from -6 to 6
- norm_gain: float32 [4096], P('chan'), may hold values from 0.25 to 1.75
Outputs:
- mixed_out: bfloat16 [1, 8192, 4096], P(None, 'time', 'chan')
The draws below stay inside these ranges and needn't reach their ends.
All inputs are finite; a program needn't handle non-finite values.
Results may differ from the reference program's by a relative error of at most 0.001.
Values sent between devices are 32-bit elements; how exact they have to be, the bound alone decides.
A program may use at most 64 MiB of HBM per device.

```python
import jax
import jax.numpy as jnp
from jax import lax

BATCH = 1
CHANNELS = 4096
LENGTH = 8192


def block_levels(rng, shape, cuts, low, largest):
    level = 1.0
    for dim, shards_of in cuts:
        draws = jax.random.uniform(jax.random.fold_in(jax.random.fold_in(rng, 6), dim), (shards_of,), jnp.float32, low / len(cuts), largest / len(cuts))
        level = level * jnp.repeat(jnp.exp(draws), shape[dim] // shards_of).reshape((-1,) + (1,) * (len(shape) - 1 - dim))
    return level


def normal_values(own_key, shape, spread, most, split=(), held_as=jnp.bfloat16):
    gain = block_levels(own_key, shape, split, -0.22, 0.18) if split else 1.0
    result = jax.random.normal(own_key, shape, jnp.float32) * spread * gain
    return jnp.minimum(jnp.maximum(result, -most), most).astype(held_as)


def setup_inputs(seed: int = 0) -> dict:
    streams_of = jax.random.split(jax.random.key(seed), 4)
    fade_rate = jnp.clip(0.2 + 1.8 * jax.random.uniform(streams_of[0], (BATCH, LENGTH, CHANNELS), jnp.float32) ** block_levels(streams_of[0], (BATCH, LENGTH, CHANNELS), ((1, 16), (2, 8)), -0.2, 0.2), 0.2, 2.0)
    update_in = normal_values(streams_of[1], (BATCH, LENGTH, CHANNELS), 1.0, 6.0, ((1, 16), (2, 8)))
    norm_gain = jnp.clip(1.0 + 0.15 * jax.random.normal(streams_of[2], (CHANNELS,), jnp.float32), 0.25, 1.75)
    return dict(fade_rate=fade_rate, update_in=update_in, norm_gain=norm_gain)


def join_pair(earlier, later):
    return (earlier[0] * later[0], later[0] * earlier[1] + later[1])

def reference(fade_rate, update_in, norm_gain):
    keep = jnp.exp(-fade_rate / LENGTH)
    push = update_in.astype(jnp.float32) * LENGTH ** (-0.5)
    forward = lax.associative_scan(join_pair, (keep, push), axis=1)[1]
    backward = lax.associative_scan(join_pair, (keep, push), axis=1, reverse=True)[1]
    states = forward + backward
    power = lax.optimization_barrier(jnp.mean(states * states, axis=-1, keepdims=True))
    mixed_out = (states * lax.rsqrt(power + 1e-06) * norm_gain).astype(jnp.bfloat16)
    return mixed_out
```

```python
import functools

import jax
import jax.numpy as jnp
from jax import lax
from jax.experimental import pallas as pl
from jax.experimental.pallas import tpu as pltpu
from jax.sharding import PartitionSpec as P

MESH = pl.DeviceIdType.MESH
LANES = 128
F32 = jnp.float32
BF16 = jnp.bfloat16


def ring_gap(step, size):
    return min(step, size - step)


def time_peers():
    offsets = [(z, y, c) for z in range(4) for y in range(2) for c in range(2)][1:]
    return sorted(offsets, key=lambda o: -(4 * ring_gap(o[0], 4) + 4 * o[1] + o[2]))


def chan_peers():
    offsets = [(y, x) for y in range(2) for x in range(4)][1:]
    return sorted(offsets, key=lambda o: -(2 * o[0] + ring_gap(o[1], 4)))


def split(value):
    high = value.astype(BF16)
    return high, (value - high.astype(F32)).astype(BF16)


def prefix(lower, value):
    block = lower.shape[0]
    carry, parts = None, []
    for start in range(0, value.shape[0], block):
        high, low = split(value[start : start + block])
        part = jnp.dot(lower, high, preferred_element_type=F32)
        part = part + jnp.dot(lower, low, preferred_element_type=F32)
        if carry is not None:
            part = part + carry
        carry = part[block - 1 : block]
        parts.append(part)
    return jnp.concatenate(parts, axis=0)


def kernel(
    sizes,
    fade_hbm,
    update_hbm,
    gain_ref,
    out_ref,
    fade,
    update,
    own,
    through,
    near,
    leave,
    message,
    inbox,
    powers,
    load_sem,
    sent_sem,
    inbox_sem,
    power_sent_sem,
    power_sem,
):
    n_time, n_chan = sizes
    rows, columns = fade.shape
    length = rows * n_time
    channels = columns * n_chan
    groups = columns // LANES
    me_t, me_c = lax.axis_index("time"), lax.axis_index("chan")

    loads = [
        pltpu.make_async_copy(fade_hbm.at[0], fade, load_sem.at[0]),
        pltpu.make_async_copy(update_hbm.at[0], update, load_sem.at[1]),
    ]
    for load in loads:
        load.start()

    z, y, core = me_t // 4, (me_t // 2) % 2, me_t % 2
    later_times = [
        ((z + dz) % 4) * 4 + ((y + dy) % 2) * 2 + (core + dc) % 2 for dz, dy, dc in time_peers()
    ]
    cy, cx = me_c // 4, me_c % 4
    other_chans = [((cy + dy) % 2) * 4 + (cx + dx) % 4 for dy, dx in chan_peers()]

    barrier = pltpu.get_barrier_semaphore()
    for peer in other_chans:
        pl.semaphore_signal(barrier, inc=1, device_id=(me_t, peer), device_id_type=MESH)
    for peer in later_times:
        pl.semaphore_signal(barrier, inc=1, device_id=(peer, me_c), device_id_type=MESH)

    half = rows // 2
    lower = (
        lax.broadcasted_iota(jnp.int32, (half, half), 0)
        >= lax.broadcasted_iota(jnp.int32, (half, half), 1)
    ).astype(BF16)

    for load in loads:
        load.wait()

    for g in range(groups):
        at = slice(g * LANES, (g + 1) * LANES)
        rate = fade[:, at] * (1.0 / length)
        push = update[:, at].astype(F32) * length**-0.5
        total = prefix(lower, rate)
        last = total[rows - 1 :]
        down = jnp.exp(-total)
        up = jnp.exp(total)
        before = total - rate
        grown = up * push
        shrunk = jnp.exp(-before) * push
        whole = jnp.exp(-last)
        message[0, 0, g : g + 1] = whole
        message[1, 0, g : g + 1] = whole
        message[0, 1, g : g + 1] = whole * jnp.sum(grown, axis=0, keepdims=True)
        message[1, 1, g : g + 1] = jnp.sum(shrunk, axis=0, keepdims=True)
        through[:, at] = down
        near[:, at] = before
        own[:, at] = grown
        leave[:, at] = shrunk

    pl.semaphore_wait(barrier, len(later_times) + len(other_chans))
    sends = []
    for peer in later_times:
        sends.append(
            pltpu.make_async_remote_copy(
                src_ref=message.at[jnp.where(peer > me_t, 0, 1)],
                dst_ref=inbox.at[me_t],
                send_sem=sent_sem,
                recv_sem=inbox_sem,
                device_id=(peer, me_c),
                device_id_type=MESH,
            )
        )
        sends[-1].start()

    for g in range(groups):
        at = slice(g * LANES, (g + 1) * LANES)
        grown, shrunk = own[:, at], leave[:, at]
        before = near[:, at]
        back = jnp.exp(before)
        ahead = jnp.sum(shrunk, axis=0, keepdims=True) - prefix(lower, shrunk) + shrunk
        own[:, at] = through[:, at] * prefix(lower, grown) + back * ahead
        near[:, at] = back * message[0, 0, g : g + 1]

    inbox[me_t] = message[0]
    pltpu.make_async_copy(
        inbox.at[pl.ds(0, n_time - 1)], inbox.at[pl.ds(0, n_time - 1)], inbox_sem
    ).wait()

    earlier = jnp.zeros((groups, LANES), F32)
    for k in range(n_time - 1):
        earlier = jnp.where(k < me_t, earlier * inbox[k, 0] + inbox[k, 1], earlier)
    later = jnp.zeros((groups, LANES), F32)
    for k in range(n_time - 1, 0, -1):
        later = jnp.where(k > me_t, later * inbox[k, 0] + inbox[k, 1], later)

    for b in range(rows // LANES):
        block = slice(b * LANES, (b + 1) * LANES)
        squares = None
        for g in range(groups):
            at = slice(g * LANES, (g + 1) * LANES)
            states = (
                own[block, at]
                + through[block, at] * earlier[g : g + 1]
                + near[block, at] * later[g : g + 1]
            )
            own[block, at] = states
            square = states * states
            squares = square if squares is None else squares + square
        powers[me_c, b : b + 1] = jnp.sum(squares.T, axis=0, keepdims=True)

    for peer in other_chans:
        sends.append(
            pltpu.make_async_remote_copy(
                src_ref=powers.at[me_c],
                dst_ref=powers.at[me_c],
                send_sem=power_sent_sem,
                recv_sem=power_sem,
                device_id=(me_t, peer),
                device_id_type=MESH,
            )
        )
        sends[-1].start()
    pltpu.make_async_copy(
        powers.at[pl.ds(0, n_chan - 1)], powers.at[pl.ds(0, n_chan - 1)], power_sem
    ).wait()

    power = powers[0]
    for k in range(1, n_chan):
        power = power + powers[k]
    scale = lax.rsqrt(power * (1.0 / channels) + 1e-06)
    for b in range(rows // LANES):
        block = slice(b * LANES, (b + 1) * LANES)
        by_row = jnp.broadcast_to(scale[b : b + 1], (LANES, LANES)).T
        for g in range(groups):
            at = slice(g * LANES, (g + 1) * LANES)
            out_ref[0, block, at] = (own[block, at] * by_row * gain_ref[:, at]).astype(BF16)

    pltpu.make_async_copy(
        inbox.at[pl.ds(0, n_time - 1)], inbox.at[pl.ds(0, n_time - 1)], sent_sem
    ).wait()
    pltpu.make_async_copy(
        powers.at[pl.ds(0, n_chan - 1)], powers.at[pl.ds(0, n_chan - 1)], power_sent_sem
    ).wait()


def per_device(fade_rate, update_in, norm_gain):
    n_time, n_chan = lax.axis_size("time"), lax.axis_size("chan")
    _, rows, columns = fade_rate.shape
    groups = columns // LANES
    return pl.pallas_call(
        functools.partial(kernel, (n_time, n_chan)),
        out_shape=jax.ShapeDtypeStruct((1, rows, columns), BF16),
        in_specs=[
            pl.BlockSpec(memory_space=pl.ANY),
            pl.BlockSpec(memory_space=pl.ANY),
            pl.BlockSpec(memory_space=pltpu.VMEM),
        ],
        out_specs=pl.BlockSpec(memory_space=pltpu.VMEM),
        scratch_shapes=[
            pltpu.VMEM((rows, columns), F32),
            pltpu.VMEM((rows, columns), BF16),
            pltpu.VMEM((rows, columns), F32),
            pltpu.VMEM((rows, columns), F32),
            pltpu.VMEM((rows, columns), F32),
            pltpu.VMEM((rows, columns), F32),
            pltpu.VMEM((2, 2, groups, LANES), F32),
            pltpu.VMEM((n_time, 2, groups, LANES), F32),
            pltpu.VMEM((n_chan, rows // LANES, LANES), F32),
            pltpu.SemaphoreType.DMA((2,)),
            pltpu.SemaphoreType.DMA,
            pltpu.SemaphoreType.DMA,
            pltpu.SemaphoreType.DMA,
            pltpu.SemaphoreType.DMA,
        ],
        compiler_params=pltpu.CompilerParams(collective_id=0, has_side_effects=True),
        name="filter_norm",
    )(fade_rate, update_in, norm_gain.reshape(1, columns))


def solution(mesh):
    return jax.shard_map(
        per_device,
        mesh=mesh,
        in_specs=(P(None, "time", "chan"), P(None, "time", "chan"), P("chan")),
        out_specs=P(None, "time", "chan"),
        check_vma=False,
    )
```

```python
import functools

import jax
import jax.numpy as jnp
from jax import lax
from jax.experimental import pallas as pl
from jax.experimental.pallas import tpu as pltpu
from jax.sharding import PartitionSpec as P

MESH = pl.DeviceIdType.MESH
LANES = 128
PITCH = 9
LOG2E = 1.4426950408889634
F32 = jnp.float32
BF16 = jnp.bfloat16


def ring_gap(step, size):
    return min(step, size - step)


def time_peers():
    offsets = [(z, y, c) for z in range(4) for y in range(2) for c in range(2)][1:]
    return sorted(offsets, key=lambda o: -(4 * ring_gap(o[0], 4) + 4 * o[1] + o[2]))


def chan_peers():
    offsets = [(y, x) for y in range(2) for x in range(4)][1:]
    return sorted(offsets, key=lambda o: -(2 * o[0] + ring_gap(o[1], 4)))


def split(value):
    high = value.astype(BF16)
    return high, (value - high.astype(F32)).astype(BF16)


def prefix(lower, value):
    block = lower.shape[0]
    carry, parts = None, []
    for start in range(0, value.shape[0], block):
        high, low = split(value[start : start + block])
        part = jnp.dot(lower, high, preferred_element_type=F32)
        part = part + jnp.dot(lower, low, preferred_element_type=F32)
        if carry is not None:
            part = part + carry
        carry = part[block - 1 : block]
        parts.append(part)
    return jnp.concatenate(parts, axis=0)


def kernel(
    sizes,
    fade_hbm,
    update_hbm,
    gain_ref,
    out_ref,
    fade,
    update,
    own,
    through,
    near,
    keeps,
    pushes,
    lower,
    message,
    inbox,
    powers,
    load_sem,
    sent_sem,
    inbox_sem,
    power_sent_sem,
    power_sem,
):
    n_time, n_chan = sizes
    groups, rows, _ = fade.shape
    columns = groups * LANES
    length = rows * n_time
    channels = columns * n_chan
    me_t, me_c = lax.axis_index("time"), lax.axis_index("chan")

    loads = []
    for g in range(groups):
        at = pl.ds(g * LANES, LANES)
        loads.append(
            (
                pltpu.make_async_copy(fade_hbm.at[0, :, at], fade.at[g], load_sem.at[0, g]),
                pltpu.make_async_copy(update_hbm.at[0, :, at], update.at[g], load_sem.at[1, g]),
            )
        )
        for load in loads[g]:
            load.start()

    z, y, core = me_t // 4, (me_t // 2) % 2, me_t % 2
    later_times = [
        ((z + dz) % 4) * 4 + ((y + dy) % 2) * 2 + (core + dc) % 2 for dz, dy, dc in time_peers()
    ]
    cy, cx = me_c // 4, me_c % 4
    other_chans = [((cy + dy) % 2) * 4 + (cx + dx) % 4 for dy, dx in chan_peers()]

    barrier = pltpu.get_barrier_semaphore()
    for peer in other_chans:
        pl.semaphore_signal(barrier, inc=1, device_id=(me_t, peer), device_id_type=MESH)
    for peer in later_times:
        pl.semaphore_signal(barrier, inc=1, device_id=(peer, me_c), device_id_type=MESH)

    half = rows // 2
    steps = half // 8

    for g in range(groups):
        for load in loads[g]:
            load.wait()
        ends = []
        summed = None
        for h in range(2):
            slab = 2 * g + h
            for i in range(0, half, 16):
                at = pl.ds(h * half + i, 16)
                rate = fade[g, at]
                keep = jnp.exp2(rate * (-LOG2E / length))
                push = update[g, at].astype(F32)
                for q in range(2):
                    run, step = divmod(i + 8 * q, steps)
                    to = pl.ds(step * PITCH + run, 8, stride=PITCH)
                    keeps[slab, to] = keep[8 * q : 8 * q + 8]
                    pushes[slab, to] = push[8 * q : 8 * q + 8]
                    part = rate[8 * q : 8 * q + 8]
                    summed = part if summed is None else summed + part
            weight = keeps[slab, pl.ds(0, 8)]
            ahead = behind = pushes[slab, pl.ds(0, 8)]
            for step in range(1, steps):
                keep = keeps[slab, pl.ds(step * PITCH, 8)]
                push = pushes[slab, pl.ds(step * PITCH, 8)]
                ahead = keep * ahead + push
                behind = behind + weight * push
                weight = weight * keep
            for gap in (1, 2, 4):
                weight_next, ahead_next, behind_next = (
                    pltpu.roll(x, 8 - gap, 0) for x in (weight, ahead, behind)
                )
                behind = behind + weight * behind_next
                ahead = ahead_next + weight_next * ahead
                weight = weight * weight_next
            ends.append((weight[:1], ahead[:1], behind[:1]))
        (weight_0, ahead_0, behind_0), (weight_1, ahead_1, behind_1) = ends
        whole = jnp.exp2(jnp.sum(summed, axis=0, keepdims=True) * (-LOG2E / length))
        message[0, 0, g : g + 1] = whole
        message[1, 0, g : g + 1] = whole
        message[0, 1, g : g + 1] = (ahead_1 + weight_1 * ahead_0) * length**-0.5
        message[1, 1, g : g + 1] = (behind_0 + weight_0 * behind_1) * length**-0.5

    pl.semaphore_wait(barrier, len(later_times) + len(other_chans))
    sends = []
    for peer in later_times:
        sends.append(
            pltpu.make_async_remote_copy(
                src_ref=message.at[jnp.where(peer > me_t, 0, 1)],
                dst_ref=inbox.at[me_t],
                send_sem=sent_sem,
                recv_sem=inbox_sem,
                device_id=(peer, me_c),
                device_id_type=MESH,
            )
        )
        sends[-1].start()

    lower[...] = (
        lax.broadcasted_iota(jnp.int32, (half, half), 0)
        >= lax.broadcasted_iota(jnp.int32, (half, half), 1)
    ).astype(BF16)

    @pl.loop(0, groups)
    def _(g):
        rate = fade[g] * (1.0 / length)
        push = update[g].astype(F32) * length**-0.5
        total = prefix(lower[...], rate)
        before = total - rate
        down = jnp.exp(-total)
        back = jnp.exp(before)
        grown = jnp.exp(total) * push
        shrunk = jnp.exp(-before) * push
        ahead = jnp.sum(shrunk, axis=0, keepdims=True) - prefix(lower[...], shrunk) + shrunk
        own[g] = down * prefix(lower[...], grown) + back * ahead
        through[g] = down
        near[g] = back * down[rows - 1 :]

    inbox[me_t] = message[0]
    pltpu.make_async_copy(
        inbox.at[pl.ds(0, n_time - 1)], inbox.at[pl.ds(0, n_time - 1)], inbox_sem
    ).wait()

    earlier = jnp.zeros((groups, LANES), F32)
    for k in range(n_time - 1):
        earlier = jnp.where(k < me_t, earlier * inbox[k, 0] + inbox[k, 1], earlier)
    later = jnp.zeros((groups, LANES), F32)
    for k in range(n_time - 1, 0, -1):
        later = jnp.where(k > me_t, later * inbox[k, 0] + inbox[k, 1], later)

    for b in range(rows // LANES):
        block = slice(b * LANES, (b + 1) * LANES)
        squares = None
        for g in range(groups):
            states = (
                own[g, block]
                + through[g, block] * earlier[g : g + 1]
                + near[g, block] * later[g : g + 1]
            )
            own[g, block] = states
            square = states * states
            squares = square if squares is None else squares + square
        powers[me_c, b : b + 1] = jnp.sum(squares.T, axis=0, keepdims=True)

    for peer in other_chans:
        sends.append(
            pltpu.make_async_remote_copy(
                src_ref=powers.at[me_c],
                dst_ref=powers.at[me_c],
                send_sem=power_sent_sem,
                recv_sem=power_sem,
                device_id=(me_t, peer),
                device_id_type=MESH,
            )
        )
        sends[-1].start()
    pltpu.make_async_copy(
        powers.at[pl.ds(0, n_chan - 1)], powers.at[pl.ds(0, n_chan - 1)], power_sem
    ).wait()

    power = powers[0]
    for k in range(1, n_chan):
        power = power + powers[k]
    scale = lax.rsqrt(power * (1.0 / channels) + 1e-06)
    for b in range(rows // LANES):
        block = slice(b * LANES, (b + 1) * LANES)
        by_row = jnp.broadcast_to(scale[b : b + 1], (LANES, LANES)).T
        for g in range(groups):
            at = slice(g * LANES, (g + 1) * LANES)
            out_ref[0, block, at] = (own[g, block] * by_row * gain_ref[:, at]).astype(BF16)

    pltpu.make_async_copy(
        inbox.at[pl.ds(0, n_time - 1)], inbox.at[pl.ds(0, n_time - 1)], sent_sem
    ).wait()
    pltpu.make_async_copy(
        powers.at[pl.ds(0, n_chan - 1)], powers.at[pl.ds(0, n_chan - 1)], power_sent_sem
    ).wait()


def per_device(fade_rate, update_in, norm_gain):
    n_time, n_chan = lax.axis_size("time"), lax.axis_size("chan")
    _, rows, columns = fade_rate.shape
    groups = columns // LANES
    return pl.pallas_call(
        functools.partial(kernel, (n_time, n_chan)),
        out_shape=pltpu.VMEM((1, rows, columns), BF16),
        in_specs=[
            pl.BlockSpec(memory_space=pl.ANY),
            pl.BlockSpec(memory_space=pl.ANY),
            pl.BlockSpec(memory_space=pltpu.VMEM),
        ],
        out_specs=pl.BlockSpec(memory_space=pltpu.VMEM),
        scratch_shapes=[
            pltpu.VMEM((groups, rows, LANES), F32),
            pltpu.VMEM((groups, rows, LANES), BF16),
            pltpu.VMEM((groups, rows, LANES), F32),
            pltpu.VMEM((groups, rows, LANES), F32),
            pltpu.VMEM((groups, rows, LANES), F32),
            pltpu.VMEM((2 * groups, rows // 16 * PITCH, LANES), F32),
            pltpu.VMEM((2 * groups, rows // 16 * PITCH, LANES), F32),
            pltpu.VMEM((rows // 2, rows // 2), BF16),
            pltpu.VMEM((2, 2, groups, LANES), F32),
            pltpu.VMEM((n_time, 2, groups, LANES), F32),
            pltpu.VMEM((n_chan, rows // LANES, LANES), F32),
            pltpu.SemaphoreType.DMA((2, groups)),
            pltpu.SemaphoreType.DMA,
            pltpu.SemaphoreType.DMA,
            pltpu.SemaphoreType.DMA,
            pltpu.SemaphoreType.DMA,
        ],
        compiler_params=pltpu.CompilerParams(collective_id=0, has_side_effects=True),
        name="filter_norm",
    )(fade_rate, update_in, norm_gain.reshape(1, columns))


def solution(mesh):
    return jax.shard_map(
        per_device,
        mesh=mesh,
        in_specs=(P(None, "time", "chan"), P(None, "time", "chan"), P("chan")),
        out_specs=P(None, "time", "chan"),
        check_vma=False,
    )
```

```python
import functools

import jax
import jax.numpy as jnp
from jax import lax
from jax.experimental import pallas as pl
from jax.experimental.pallas import tpu as pltpu
from jax.sharding import PartitionSpec as P

MESH = pl.DeviceIdType.MESH
LANES = 128
RUNS = 8
PITCH = 9
LOG2E = 1.4426950408889634
F32 = jnp.float32
BF16 = jnp.bfloat16


def ring_gap(step, size):
    return min(step, size - step)


def time_peers():
    offsets = [(z, y, c) for z in range(4) for y in range(2) for c in range(2)][1:]
    return sorted(offsets, key=lambda o: -(4 * ring_gap(o[0], 4) + 4 * o[1] + o[2]))


def chan_peers():
    offsets = [(y, x) for y in range(2) for x in range(4)][1:]
    return sorted(offsets, key=lambda o: -(2 * o[0] + ring_gap(o[1], 4)))


def scan_runs(weight, value, down):
    run = lax.broadcasted_iota(jnp.int32, weight.shape, 0)
    run = run if down else RUNS - 1 - run
    for gap in (1, 2, 4):
        shift = gap if down else RUNS - gap
        value = value + weight * jnp.where(run >= gap, pltpu.roll(value, shift, 0), 0.0)
        weight = weight * jnp.where(run >= gap, pltpu.roll(weight, shift, 0), 1.0)
    end = slice(RUNS - 1, RUNS) if down else slice(0, 1)
    shift = 1 if down else RUNS - 1
    weight_in = jnp.where(run >= 1, pltpu.roll(weight, shift, 0), 1.0)
    value_in = jnp.where(run >= 1, pltpu.roll(value, shift, 0), 0.0)
    return weight_in, value_in, weight[end], value[end]


def states_kernel(
    sizes,
    fade_hbm,
    update_hbm,
    gain_hbm,
    states,
    power_ref,
    gain,
    fade,
    update,
    keeps,
    pushes,
    own,
    through,
    near,
    runs,
    message,
    inbox,
    powers,
    load_sem,
    gain_sem,
    sent_sem,
    inbox_sem,
    power_sent_sem,
    power_sem,
):
    n_time, n_chan = sizes
    groups, rows, _ = fade.shape
    length = rows * n_time
    half = rows // 2
    steps = half // RUNS
    me_t, me_c = lax.axis_index("time"), lax.axis_index("chan")

    loads = []
    for g in range(groups):
        at = pl.ds(g * LANES, LANES)
        loads.append(
            (
                pltpu.make_async_copy(fade_hbm.at[0, :, at], fade.at[g], load_sem.at[0, g]),
                pltpu.make_async_copy(update_hbm.at[0, :, at], update.at[g], load_sem.at[1, g]),
            )
        )
        for load in loads[g]:
            load.start()
    gain_load = pltpu.make_async_copy(gain_hbm, gain, gain_sem)
    gain_load.start()

    z, y, core = me_t // 4, (me_t // 2) % 2, me_t % 2
    other_times = [
        ((z + dz) % 4) * 4 + ((y + dy) % 2) * 2 + (core + dc) % 2 for dz, dy, dc in time_peers()
    ]
    cy, cx = me_c // 4, me_c % 4
    other_chans = [((cy + dy) % 2) * 4 + (cx + dx) % 4 for dy, dx in chan_peers()]

    barrier = pltpu.get_barrier_semaphore()
    for peer in other_chans:
        pl.semaphore_signal(barrier, inc=1, device_id=(me_t, peer), device_id_type=MESH)
    for peer in other_times:
        pl.semaphore_signal(barrier, inc=1, device_id=(peer, me_c), device_id_type=MESH)

    for g in range(groups):
        for load in loads[g]:
            load.wait()
        ends = []
        summed = None
        for h in range(2):
            slab = 2 * g + h
            for i in range(0, half, 16):
                at = pl.ds(h * half + i, 16)
                rate = fade[g, at]
                keep = jnp.exp2(rate * (-LOG2E / length))
                push = update[g, at].astype(F32)
                for q in range(2):
                    run, step = divmod(i + 8 * q, steps)
                    to = pl.ds(step * PITCH + run, 8, stride=PITCH)
                    keeps[slab, to] = keep[8 * q : 8 * q + 8]
                    pushes[slab, to] = push[8 * q : 8 * q + 8]
                    part = rate[8 * q : 8 * q + 8]
                    summed = part if summed is None else summed + part
            weight = keeps[slab, pl.ds(0, RUNS)]
            ahead = behind = pushes[slab, pl.ds(0, RUNS)]
            for step in range(1, steps):
                keep = keeps[slab, pl.ds(step * PITCH, RUNS)]
                push = pushes[slab, pl.ds(step * PITCH, RUNS)]
                ahead = keep * ahead + push
                behind = behind + weight * push
                weight = weight * keep
            runs[slab, 0] = weight
            runs[slab, 1] = ahead
            runs[slab, 2] = behind
            for gap in (1, 2, 4):
                weight_next, ahead_next, behind_next = (
                    pltpu.roll(x, RUNS - gap, 0) for x in (weight, ahead, behind)
                )
                behind = behind + weight * behind_next
                ahead = ahead_next + weight_next * ahead
                weight = weight * weight_next
            ends.append((weight[:1], ahead[:1], behind[:1]))
        (weight_0, ahead_0, behind_0), (weight_1, ahead_1, behind_1) = ends
        whole = jnp.exp2(jnp.sum(summed, axis=0, keepdims=True) * (-LOG2E / length))
        message[0, 0, g : g + 1] = whole
        message[1, 0, g : g + 1] = whole
        message[0, 1, g : g + 1] = ahead_1 + weight_1 * ahead_0
        message[1, 1, g : g + 1] = behind_0 + weight_0 * behind_1

    pl.semaphore_wait(barrier, len(other_times) + len(other_chans))
    for peer in other_times:
        pltpu.make_async_remote_copy(
            src_ref=message.at[jnp.where(peer > me_t, 0, 1)],
            dst_ref=inbox.at[me_t],
            send_sem=sent_sem,
            recv_sem=inbox_sem.at[me_t],
            device_id=(peer, me_c),
            device_id_type=MESH,
        ).start()

    @pl.loop(0, groups)
    def _(g):
        slabs = (2 * g, 2 * g + 1)
        weights, aheads, behinds = ([runs[slab, k] for slab in slabs] for k in range(3))
        down_0, ahead_0, down_all, ahead_all = scan_runs(weights[0], aheads[0], True)
        down_1, ahead_1, _, _ = scan_runs(weights[1], aheads[1], True)
        up_1, behind_1, up_all, behind_all = scan_runs(weights[1], behinds[1], False)
        up_0, behind_0, _, _ = scan_runs(weights[0], behinds[0], False)
        ahead = [ahead_0, ahead_1 + down_1 * ahead_all]
        down = [down_0, down_1 * down_all]
        behind = [behind_0 + up_0 * behind_all, behind_1]
        up = [up_0 * up_all, up_1]
        for step in range(steps):
            at = pl.ds(step * PITCH, RUNS)
            for h, slab in enumerate(slabs):
                keep = keeps[slab, at]
                ahead[h] = keep * ahead[h] + pushes[slab, at]
                down[h] = keep * down[h]
                own[slab, at] = ahead[h]
                through[slab, at] = down[h]
        for step in range(steps - 1, -1, -1):
            at = pl.ds(step * PITCH, RUNS)
            for h, slab in enumerate(slabs):
                keep = keeps[slab, at]
                behind[h] = keep * behind[h] + pushes[slab, at]
                up[h] = keep * up[h]
                own[slab, at] = own[slab, at] + behind[h]
                near[slab, at] = up[h]

    def taken(k, state):
        pltpu.make_async_copy(inbox.at[k], inbox.at[k], inbox_sem.at[k]).wait()
        return state * inbox[k, 0] + inbox[k, 1]

    zero = jnp.zeros((groups, LANES), F32)
    earlier = lax.fori_loop(0, me_t, taken, zero)
    for g in range(groups):
        entering = jnp.broadcast_to(earlier[g : g + 1], (RUNS, LANES))
        for slab in (2 * g, 2 * g + 1):
            for step in range(steps):
                at = pl.ds(step * PITCH, RUNS)
                own[slab, at] = own[slab, at] + through[slab, at] * entering

    later = lax.fori_loop(0, n_time - 1 - me_t, lambda i, state: taken(n_time - 1 - i, state), zero)

    entering = [jnp.broadcast_to(later[g : g + 1], (RUNS, LANES)) for g in range(groups)]
    for b in range(rows // LANES):
        squares = []
        for row in range(b * LANES, (b + 1) * LANES, 8):
            h, place = divmod(row, half)
            run, step = divmod(place, steps)
            at = pl.ds(step * PITCH + run, 8, stride=PITCH)
            total = None
            for g in range(groups):
                state = own[2 * g + h, at] + near[2 * g + h, at] * entering[g]
                states[g, pl.ds(row, 8)] = state
                square = state * state
                total = square if total is None else total + square
            squares.append(total)
        powers[me_c, b : b + 1] = jnp.sum(jnp.concatenate(squares, axis=0).T, axis=0, keepdims=True)

    for peer in other_chans:
        pltpu.make_async_remote_copy(
            src_ref=powers.at[me_c],
            dst_ref=powers.at[me_c],
            send_sem=power_sent_sem,
            recv_sem=power_sem,
            device_id=(me_t, peer),
            device_id_type=MESH,
        ).start()
    others = powers.at[pl.ds(0, n_chan - 1)]
    pltpu.make_async_copy(others, others, power_sem).wait()
    power = powers[0]
    for k in range(1, n_chan):
        power = power + powers[k]
    power_ref[...] = power

    gain_load.wait()
    others = inbox.at[pl.ds(0, n_time - 1)]
    pltpu.make_async_copy(others, others, sent_sem).wait()
    others = powers.at[pl.ds(0, n_chan - 1)]
    pltpu.make_async_copy(others, others, power_sent_sem).wait()


def norm_kernel(sizes, states, power, gain, out_hbm, out, out_sem):
    channels, length = sizes
    groups, rows, _ = states.shape
    scale = lax.rsqrt(power[...] * (1.0 / channels) + 1e-06 * length)
    stores = []
    for b in range(rows // LANES):
        block = pl.ds(b * LANES, LANES)
        by_row = jnp.broadcast_to(scale[b : b + 1], (LANES, LANES)).T
        for g in range(groups):
            at = pl.ds(g * LANES, LANES)
            out[block, at] = (states[g, block] * by_row * gain[:, at]).astype(BF16)
        stores.append(pltpu.make_async_copy(out.at[block], out_hbm.at[0, block], out_sem.at[b]))
        stores[b].start()
    for store in stores:
        store.wait()


def per_device(fade_rate, update_in, norm_gain):
    n_time, n_chan = lax.axis_size("time"), lax.axis_size("chan")
    _, rows, columns = fade_rate.shape
    groups = columns // LANES
    anywhere = pl.BlockSpec(memory_space=pl.ANY)
    vmem = pl.BlockSpec(memory_space=pltpu.VMEM)
    slabs = pltpu.VMEM((2 * groups, rows // (2 * RUNS) * PITCH, LANES), F32)
    states, power, gain = pl.pallas_call(
        functools.partial(states_kernel, (n_time, n_chan)),
        out_shape=(
            pltpu.VMEM((groups, rows, LANES), F32),
            pltpu.VMEM((rows // LANES, LANES), F32),
            pltpu.VMEM((1, columns), F32),
        ),
        in_specs=[anywhere, anywhere, anywhere],
        out_specs=(vmem, vmem, vmem),
        scratch_shapes=[
            pltpu.VMEM((groups, rows, LANES), F32),
            pltpu.VMEM((groups, rows, LANES), BF16),
            slabs,
            slabs,
            slabs,
            slabs,
            slabs,
            pltpu.VMEM((2 * groups, 3, RUNS, LANES), F32),
            pltpu.VMEM((2, 2, groups, LANES), F32),
            pltpu.VMEM((n_time, 2, groups, LANES), F32),
            pltpu.VMEM((n_chan, rows // LANES, LANES), F32),
            pltpu.SemaphoreType.DMA((2, groups)),
            pltpu.SemaphoreType.DMA,
            pltpu.SemaphoreType.DMA,
            pltpu.SemaphoreType.DMA((n_time,)),
            pltpu.SemaphoreType.DMA,
            pltpu.SemaphoreType.DMA,
        ],
        compiler_params=pltpu.CompilerParams(collective_id=0, has_side_effects=True),
        name="filter_states",
    )(fade_rate, update_in, norm_gain.reshape(1, columns))
    states, power, gain = (
        pltpu.with_memory_space_constraint(x, pltpu.VMEM) for x in (states, power, gain)
    )
    return pl.pallas_call(
        functools.partial(norm_kernel, (columns * n_chan, rows * n_time)),
        out_shape=jax.ShapeDtypeStruct((1, rows, columns), BF16),
        in_specs=[vmem, vmem, vmem],
        out_specs=anywhere,
        scratch_shapes=[
            pltpu.VMEM((rows, columns), BF16),
            pltpu.SemaphoreType.DMA((rows // LANES,)),
        ],
        name="channel_norm",
    )(states, power, gain)


def solution(mesh):
    return jax.shard_map(
        per_device,
        mesh=mesh,
        in_specs=(P(None, "time", "chan"), P(None, "time", "chan"), P("chan")),
        out_specs=P(None, "time", "chan"),
        check_vma=False,
    )
```

```python
import functools

import jax
import jax.numpy as jnp
from jax import lax
from jax.experimental import pallas as pl
from jax.experimental.pallas import tpu as pltpu
from jax.sharding import PartitionSpec as P

MESH = pl.DeviceIdType.MESH
LANES = 128
RUNS = 8
PITCH = 9
LOG2E = 1.4426950408889634
F32 = jnp.float32
BF16 = jnp.bfloat16


def ring_gap(step, size):
    return min(step, size - step)


def time_peers():
    offsets = [(z, y, c) for z in range(4) for y in range(2) for c in range(2)][1:]
    return sorted(offsets, key=lambda o: -(4 * ring_gap(o[0], 4) + 4 * o[1] + o[2]))


def chan_peers():
    offsets = [(y, x) for y in range(2) for x in range(4)][1:]
    return sorted(offsets, key=lambda o: -(2 * o[0] + ring_gap(o[1], 4)))


def scan_runs(weight, value, down):
    run = lax.broadcasted_iota(jnp.int32, weight.shape, 0)
    run = run if down else RUNS - 1 - run
    for gap in (1, 2, 4):
        shift = gap if down else RUNS - gap
        value = value + weight * jnp.where(run >= gap, pltpu.roll(value, shift, 0), 0.0)
        weight = weight * jnp.where(run >= gap, pltpu.roll(weight, shift, 0), 1.0)
    end = slice(RUNS - 1, RUNS) if down else slice(0, 1)
    shift = 1 if down else RUNS - 1
    weight_in = jnp.where(run >= 1, pltpu.roll(weight, shift, 0), 1.0)
    value_in = jnp.where(run >= 1, pltpu.roll(value, shift, 0), 0.0)
    return weight_in, value_in, weight[end], value[end]


def arrived(like, sem):
    pltpu.make_async_copy(like, like, sem).wait()


def states_kernel(
    sizes,
    fade_hbm,
    update_hbm,
    gain_hbm,
    states,
    power_ref,
    gain,
    fade,
    update,
    keeps,
    pushes,
    own,
    through,
    near,
    runs,
    message,
    inbox,
    powers,
    load_sem,
    gain_sem,
    sent_sem,
    inbox_sem,
    power_sem,
    near_sem,
    far_sem,
):
    n_time, n_chan = sizes
    groups, rows, _ = fade.shape
    length = rows * n_time
    half = rows // 2
    steps = half // RUNS
    me_t, me_c = lax.axis_index("time"), lax.axis_index("chan")

    for g in range(groups):
        at = pl.ds(g * LANES, LANES)
        pltpu.make_async_copy(fade_hbm.at[0, :, at], fade.at[g], load_sem.at[g]).start()
        pltpu.make_async_copy(update_hbm.at[0, :, at], update.at[g], load_sem.at[g]).start()
    gain_load = pltpu.make_async_copy(gain_hbm, gain, gain_sem)
    gain_load.start()

    z, y, core = me_t // 4, (me_t // 2) % 2, me_t % 2
    other_times = [
        ((z + dz) % 4) * 4 + ((y + dy) % 2) * 2 + (core + dc) % 2 for dz, dy, dc in time_peers()
    ]
    cy, cx = me_c // 4, me_c % 4
    other_chans = [((cy + dy) % 2) * 4 + (cx + dx) % 4 for dy, dx in chan_peers()]

    neighbours = [cy * 4 + (cx + 1) % 4, cy * 4 + (cx + 3) % 4, (1 - cy) * 4 + cx]

    barrier = pltpu.get_barrier_semaphore()
    for peer in neighbours:
        pl.semaphore_signal(barrier, inc=1, device_id=(me_t, peer), device_id_type=MESH)
    for peer in other_times:
        pl.semaphore_signal(barrier, inc=1, device_id=(peer, me_c), device_id_type=MESH)

    for g in range(groups):
        arrived(fade.at[pl.ds(0, 3), pl.ds(0, half)], load_sem.at[g])
        ends = []
        summed = None
        for h in range(2):
            slab = 2 * g + h
            for i in range(0, half, 16):
                at = pl.ds(h * half + i, 16)
                rate = fade[g, at]
                keep = jnp.exp2(rate * (-LOG2E / length))
                push = update[g, at].astype(F32)
                for q in range(2):
                    run, step = divmod(i + 8 * q, steps)
                    to = pl.ds(step * PITCH + run, 8, stride=PITCH)
                    keeps[slab, to] = keep[8 * q : 8 * q + 8]
                    pushes[slab, to] = push[8 * q : 8 * q + 8]
                    part = rate[8 * q : 8 * q + 8]
                    summed = part if summed is None else summed + part
            weight = keeps[slab, pl.ds(0, RUNS)]
            ahead = behind = pushes[slab, pl.ds(0, RUNS)]
            for step in range(1, steps):
                keep = keeps[slab, pl.ds(step * PITCH, RUNS)]
                push = pushes[slab, pl.ds(step * PITCH, RUNS)]
                ahead = keep * ahead + push
                behind = behind + weight * push
                weight = weight * keep
            runs[slab, 0] = weight
            runs[slab, 1] = ahead
            runs[slab, 2] = behind
            for gap in (1, 2, 4):
                weight_next, ahead_next, behind_next = (
                    pltpu.roll(x, RUNS - gap, 0) for x in (weight, ahead, behind)
                )
                behind = behind + weight * behind_next
                ahead = ahead_next + weight_next * ahead
                weight = weight * weight_next
            ends.append((weight[:1], ahead[:1], behind[:1]))
        (weight_0, ahead_0, behind_0), (weight_1, ahead_1, behind_1) = ends
        whole = jnp.exp2(jnp.sum(summed, axis=0, keepdims=True) * (-LOG2E / length))
        message[0, 0, g : g + 1] = whole
        message[1, 0, g : g + 1] = whole
        message[0, 1, g : g + 1] = ahead_1 + weight_1 * ahead_0
        message[1, 1, g : g + 1] = behind_0 + weight_0 * behind_1

    pl.semaphore_wait(barrier, len(other_times) + len(neighbours))
    for peer in other_times:
        pltpu.make_async_remote_copy(
            src_ref=message.at[jnp.where(peer > me_t, 0, 1)],
            dst_ref=inbox.at[me_t],
            send_sem=sent_sem,
            recv_sem=inbox_sem.at[jnp.where(peer > me_t, 0, 1)],
            device_id=(peer, me_c),
            device_id_type=MESH,
        ).start()

    for peer in neighbours:
        pl.semaphore_signal(near_sem, inc=1, device_id=(me_t, peer), device_id_type=MESH)

    @pl.loop(0, groups)
    def _(g):
        slabs = (2 * g, 2 * g + 1)
        weights, aheads, behinds = ([runs[slab, k] for slab in slabs] for k in range(3))
        down_0, ahead_0, down_all, ahead_all = scan_runs(weights[0], aheads[0], True)
        down_1, ahead_1, _, _ = scan_runs(weights[1], aheads[1], True)
        up_1, behind_1, up_all, behind_all = scan_runs(weights[1], behinds[1], False)
        up_0, behind_0, _, _ = scan_runs(weights[0], behinds[0], False)
        ahead = [ahead_0, ahead_1 + down_1 * ahead_all]
        down = [down_0, down_1 * down_all]
        behind = [behind_0 + up_0 * behind_all, behind_1]
        up = [up_0 * up_all, up_1]
        for step in range(steps):
            at = pl.ds(step * PITCH, RUNS)
            for h, slab in enumerate(slabs):
                keep = keeps[slab, at]
                ahead[h] = keep * ahead[h] + pushes[slab, at]
                down[h] = keep * down[h]
                own[slab, at] = ahead[h]
                through[slab, at] = down[h]
        for step in range(steps - 1, -1, -1):
            at = pl.ds(step * PITCH, RUNS)
            for h, slab in enumerate(slabs):
                keep = keeps[slab, at]
                behind[h] = keep * behind[h] + pushes[slab, at]
                up[h] = keep * up[h]
                own[slab, at] = own[slab, at] + behind[h]
                near[slab, at] = up[h]

    pl.semaphore_wait(near_sem, len(neighbours))
    for peer in neighbours:
        pl.semaphore_signal(far_sem, inc=1, device_id=(me_t, peer), device_id_type=MESH)

    def taken(k, state):
        return state * inbox[k, 0] + inbox[k, 1]

    for k in range(1, n_time):

        @pl.when(me_t == k)
        def _():
            arrived(inbox.at[pl.ds(0, k)], inbox_sem.at[0])

    zero = jnp.zeros((groups, LANES), F32)
    earlier = lax.fori_loop(0, me_t, taken, zero)
    for g in range(groups):
        entering = jnp.broadcast_to(earlier[g : g + 1], (RUNS, LANES))
        for slab in (2 * g, 2 * g + 1):
            for step in range(steps):
                at = pl.ds(step * PITCH, RUNS)
                own[slab, at] = own[slab, at] + through[slab, at] * entering

    for k in range(1, n_time):

        @pl.when(me_t == n_time - 1 - k)
        def _():
            arrived(inbox.at[pl.ds(0, k)], inbox_sem.at[1])

    later = lax.fori_loop(0, n_time - 1 - me_t, lambda i, state: taken(n_time - 1 - i, state), zero)

    entering = [jnp.broadcast_to(later[g : g + 1], (RUNS, LANES)) for g in range(groups)]
    for b in range(rows // LANES):
        squares = []
        for row in range(b * LANES, (b + 1) * LANES, 8):
            h, place = divmod(row, half)
            run, step = divmod(place, steps)
            at = pl.ds(step * PITCH + run, 8, stride=PITCH)
            total = None
            for g in range(groups):
                state = own[2 * g + h, at] + near[2 * g + h, at] * entering[g]
                states[g, pl.ds(row, 8)] = state
                square = state * state
                total = square if total is None else total + square
            squares.append(total)
        powers[me_c, b : b + 1] = jnp.sum(jnp.concatenate(squares, axis=0).T, axis=0, keepdims=True)

    pl.semaphore_wait(far_sem, len(neighbours))
    for peer in other_chans:
        pltpu.make_async_remote_copy(
            src_ref=powers.at[me_c],
            dst_ref=powers.at[me_c],
            send_sem=sent_sem,
            recv_sem=power_sem,
            device_id=(me_t, peer),
            device_id_type=MESH,
        ).start()
    arrived(powers.at[pl.ds(0, n_chan - 1)], power_sem)
    power = powers[0]
    for k in range(1, n_chan):
        power = power + powers[k]
    power_ref[...] = power

    gain_load.wait()
    sent = 2 * groups * (n_time - 1) + rows // LANES * (n_chan - 1)
    arrived(fade.at[0, pl.ds(0, sent)], sent_sem)


def norm_kernel(sizes, states, power, gain, out_hbm, out, out_sem):
    channels, length = sizes
    groups, rows, _ = states.shape
    scale = lax.rsqrt(power[...] * (1.0 / channels) + 1e-06 * length)
    stores = []
    for b in range(rows // LANES):
        block = pl.ds(b * LANES, LANES)
        by_row = jnp.broadcast_to(scale[b : b + 1], (LANES, LANES)).T
        for g in range(groups):
            at = pl.ds(g * LANES, LANES)
            out[block, at] = (states[g, block] * by_row * gain[:, at]).astype(BF16)
        stores.append(pltpu.make_async_copy(out.at[block], out_hbm.at[0, block], out_sem.at[b]))
        stores[b].start()
    for store in stores:
        store.wait()


def per_device(fade_rate, update_in, norm_gain):
    n_time, n_chan = lax.axis_size("time"), lax.axis_size("chan")
    _, rows, columns = fade_rate.shape
    groups = columns // LANES
    anywhere = pl.BlockSpec(memory_space=pl.ANY)
    vmem = pl.BlockSpec(memory_space=pltpu.VMEM)
    slabs = pltpu.VMEM((2 * groups, rows // (2 * RUNS) * PITCH, LANES), F32)
    states, power, gain = pl.pallas_call(
        functools.partial(states_kernel, (n_time, n_chan)),
        out_shape=(
            pltpu.VMEM((groups, rows, LANES), F32),
            pltpu.VMEM((rows // LANES, LANES), F32),
            pltpu.VMEM((1, columns), F32),
        ),
        in_specs=[anywhere, anywhere, anywhere],
        out_specs=(vmem, vmem, vmem),
        scratch_shapes=[
            pltpu.VMEM((groups, rows, LANES), F32),
            pltpu.VMEM((groups, rows, LANES), BF16),
            slabs,
            slabs,
            slabs,
            slabs,
            slabs,
            pltpu.VMEM((2 * groups, 3, RUNS, LANES), F32),
            pltpu.VMEM((2, 2, groups, LANES), F32),
            pltpu.VMEM((n_time, 2, groups, LANES), F32),
            pltpu.VMEM((n_chan, rows // LANES, LANES), F32),
            pltpu.SemaphoreType.DMA((groups,)),
            pltpu.SemaphoreType.DMA,
            pltpu.SemaphoreType.DMA,
            pltpu.SemaphoreType.DMA((2,)),
            pltpu.SemaphoreType.DMA,
            pltpu.SemaphoreType.REGULAR,
            pltpu.SemaphoreType.REGULAR,
        ],
        compiler_params=pltpu.CompilerParams(collective_id=0, has_side_effects=True),
        name="filter_states",
    )(fade_rate, update_in, norm_gain.reshape(1, columns))
    states, power, gain = (
        pltpu.with_memory_space_constraint(x, pltpu.VMEM) for x in (states, power, gain)
    )
    return pl.pallas_call(
        functools.partial(norm_kernel, (columns * n_chan, rows * n_time)),
        out_shape=jax.ShapeDtypeStruct((1, rows, columns), BF16),
        in_specs=[vmem, vmem, vmem],
        out_specs=anywhere,
        scratch_shapes=[
            pltpu.VMEM((rows, columns), BF16),
            pltpu.SemaphoreType.DMA((rows // LANES,)),
        ],
        name="channel_norm",
    )(states, power, gain)


def solution(mesh):
    return jax.shard_map(
        per_device,
        mesh=mesh,
        in_specs=(P(None, "time", "chan"), P(None, "time", "chan"), P("chan")),
        out_specs=P(None, "time", "chan"),
        check_vma=False,
    )
```

```python
import functools

import jax
import jax.numpy as jnp
from jax import lax
from jax.experimental import pallas as pl
from jax.experimental.pallas import tpu as pltpu
from jax.sharding import PartitionSpec as P

MESH = pl.DeviceIdType.MESH
LANES = 128
RUNS = 8
PIECES = 4
PLANE = 4
CHAN_RING = 4
PITCH = 17
LOG2E = 1.4426950408889634
F32 = jnp.float32
BF16 = jnp.bfloat16


def scan_runs(weight, value, down):
    run = lax.broadcasted_iota(jnp.int32, weight.shape, 0)
    run = run if down else RUNS - 1 - run
    for gap in (1, 2, 4):
        shift = gap if down else RUNS - gap
        value = value + weight * jnp.where(run >= gap, pltpu.roll(value, shift, 0), 0.0)
        weight = weight * jnp.where(run >= gap, pltpu.roll(weight, shift, 0), 1.0)
    shift = 1 if down else RUNS - 1
    weight = jnp.where(run >= 1, pltpu.roll(weight, shift, 0), 1.0)
    return weight, jnp.where(run >= 1, pltpu.roll(value, shift, 0), 0.0)


def arrived(like, sem):
    pltpu.make_async_copy(like, like, sem).wait()


def told(sem, times):
    @pl.when(times > 0)
    def _():
        pl.semaphore_wait(sem, times)


def states_kernel(
    sizes,
    fade_hbm,
    update_hbm,
    gain_hbm,
    states,
    power_ref,
    fade,
    update,
    gain,
    flows,
    own,
    through,
    pieces,
    runs,
    message,
    inbox,
    powers,
    load_sem,
    gain_sem,
    sent_sem,
    inbox_sem,
    power_sem,
    come_sem,
    near_sem,
    middle_sem,
    far_sem,
):
    n_time, n_chan = sizes
    groups, rows, _ = fade.shape
    length = rows * n_time
    steps = rows // (RUNS * PIECES)
    for g in range(groups):
        at = pl.ds(g * LANES, LANES)
        pltpu.make_async_copy(fade_hbm.at[0, :, at], fade.at[g], load_sem.at[g]).start()
        pltpu.make_async_copy(update_hbm.at[0, :, at], update.at[g], load_sem.at[g]).start()
    gain_load = pltpu.make_async_copy(gain_hbm, gain, gain_sem)
    gain_load.start()
    pl.delay(1)

    me_t, me_c = lax.axis_index("time"), lax.axis_index("chan")
    row, cx = me_c // CHAN_RING, me_c % CHAN_RING
    around = [
        row * CHAN_RING + (cx + 1) % CHAN_RING,
        row * CHAN_RING + (cx + CHAN_RING - 1) % CHAN_RING,
        me_c + CHAN_RING - 2 * CHAN_RING * row,
    ]
    plane = me_t // PLANE
    lower_around = sum(jnp.where(peer < me_c, 1, 0) for peer in around)

    barrier = pltpu.get_barrier_semaphore()
    for peer in around:

        @pl.when(peer > me_c)
        def _():
            pl.semaphore_signal(barrier, inc=1, device_id=(me_t, peer), device_id_type=MESH)

    @pl.loop(me_t + 1, n_time)
    def _(k):
        pl.semaphore_signal(barrier, inc=1, device_id=(k, me_c), device_id_type=MESH)

    def spread(g):
        summed = None
        for i in range(0, rows, 16):
            at = pl.ds(i, 16)
            rate = fade[g, at]
            keep = jnp.exp2(rate * (-LOG2E / length))
            part = rate[:8] + rate[8:]
            summed = part if summed is None else summed + part
            push = update[g, at].astype(F32)
            for q in range(2):
                run, place = divmod(i + 8 * q, rows // RUNS)
                piece, step = divmod(place, steps)
                to = pl.ds(step * PITCH + run, 8, stride=PITCH)
                to_push = pl.ds(step * PITCH + RUNS + run, 8, stride=PITCH)
                flows[g * PIECES + piece, to] = keep[8 * q : 8 * q + 8]
                flows[g * PIECES + piece, to_push] = push[8 * q : 8 * q + 8]
        whole = jnp.exp2(jnp.sum(summed, axis=0, keepdims=True) * (-LOG2E / length))
        message[0, 0, g : g + 1] = whole
        message[1, 0, g : g + 1] = whole

    def summary(g):
        slabs = range(g * PIECES, (g + 1) * PIECES)
        weights = [flows[slab, pl.ds(0, RUNS)] for slab in slabs]
        aheads = [flows[slab, pl.ds(RUNS, RUNS)] for slab in slabs]
        behinds = list(aheads)
        for step in range(1, steps):
            at, at_push = pl.ds(step * PITCH, RUNS), pl.ds(step * PITCH + RUNS, RUNS)
            for p, slab in enumerate(slabs):
                keep, push = flows[slab, at], flows[slab, at_push]
                aheads[p] = keep * aheads[p] + push
                behinds[p] = behinds[p] + weights[p] * push
                weights[p] = weights[p] * keep
        for p, slab in enumerate(slabs):
            pieces[slab, 0], pieces[slab, 1], pieces[slab, 2] = weights[p], aheads[p], behinds[p]
        parts = list(zip(weights, aheads, behinds))
        while len(parts) > 1:
            parts = [
                (w0 * w1, a1 + w1 * a0, b0 + w0 * b1)
                for (w0, a0, b0), (w1, a1, b1) in zip(parts[::2], parts[1::2])
            ]
        weight, ahead, behind = parts[0]
        runs[g, 0], runs[g, 1], runs[g, 2] = weight, ahead, behind
        for gap in (1, 2, 4):
            weight_next, ahead_next, behind_next = (
                pltpu.roll(x, RUNS - gap, 0) for x in (weight, ahead, behind)
            )
            behind = behind + weight * behind_next
            ahead = ahead_next + weight_next * ahead
            weight = weight * weight_next
        message[0, 1, g : g + 1] = ahead[:1]
        message[1, 1, g : g + 1] = behind[:1]

    for g in range(groups + 1):
        if g < groups:
            arrived(fade.at[pl.ds(0, 3), pl.ds(0, rows // 2)], load_sem.at[g])
            spread(g)
        if g > 0:
            summary(g - 1)

    def send_summary(k, way):
        pltpu.make_async_remote_copy(
            src_ref=message.at[way],
            dst_ref=inbox.at[me_t],
            send_sem=sent_sem,
            recv_sem=inbox_sem.at[way],
            device_id=(k, me_c),
            device_id_type=MESH,
        ).start()

    told(barrier, me_t + lower_around)
    @pl.loop(0, me_t)
    def _(k):
        send_summary(k, 1)

    for peer in around:

        @pl.when(peer < me_c)
        def _():
            pl.semaphore_signal(near_sem, inc=1, device_id=(me_t, peer), device_id_type=MESH)

    @pl.loop(0, me_t)
    def _(k):
        come = come_sem.at[plane]
        pl.semaphore_signal(come, inc=1, device_id=(k, me_c), device_id_type=MESH)

    told(come_sem.at[plane], PLANE - 1 - me_t % PLANE)

    @pl.loop(me_t + 1, (plane + 1) * PLANE)
    def _(k):
        send_summary(k, 0)

    def send_plane(to):
        @pl.when(to > plane)
        def _():
            pl.semaphore_wait(come_sem.at[to], PLANE)
            for k in range(to * PLANE, (to + 1) * PLANE):
                send_summary(k, 0)

    def tell_around(sem):
        for peer in around:
            pl.semaphore_signal(sem, inc=1, device_id=(me_t, peer), device_id_type=MESH)

    @pl.loop(0, groups)
    def _(g):
        slabs = [g * PIECES + p for p in range(PIECES)]
        down_in, ahead_in = scan_runs(runs[g, 0], runs[g, 1], True)
        up_in, behind_in = scan_runs(runs[g, 0], runs[g, 2], False)
        down, ahead, up, behind = [], [], [], []
        for slab in slabs:
            down.append(down_in)
            ahead.append(ahead_in)
            down_in = down_in * pieces[slab, 0]
            ahead_in = ahead_in * pieces[slab, 0] + pieces[slab, 1]
        for slab in slabs[::-1]:
            up.insert(0, up_in)
            behind.insert(0, behind_in)
            up_in = up_in * pieces[slab, 0]
            behind_in = behind_in * pieces[slab, 0] + pieces[slab, 2]
        for step in range(steps):
            at, at_2 = pl.ds(step * PITCH, RUNS), pl.ds(step * PITCH + RUNS, RUNS)
            for p, slab in enumerate(slabs):
                keep = flows[slab, at]
                ahead[p] = keep * ahead[p] + flows[slab, at_2]
                down[p] = keep * down[p]
                own[slab, at] = ahead[p]
                through[slab, at] = down[p]
        for step in range(steps - 1, -1, -1):
            at, at_2 = pl.ds(step * PITCH, RUNS), pl.ds(step * PITCH + RUNS, RUNS)
            for p, slab in enumerate(slabs):
                keep = flows[slab, at]
                behind[p] = keep * behind[p] + flows[slab, at_2]
                up[p] = keep * up[p]
                own[slab, at] = own[slab, at] + behind[p]
                own[slab, at_2] = up[p]

    told(near_sem, len(around) - lower_around)
    tell_around(middle_sem)
    for to in range(1, n_time // PLANE):
        send_plane(to)
    pl.semaphore_wait(middle_sem, len(around))
    tell_around(far_sem)

    def taken(k, state):
        return state * inbox[k, 0] + inbox[k, 1]

    for k in range(1, n_time):

        @pl.when(me_t == k)
        def _():
            arrived(inbox.at[pl.ds(0, k)], inbox_sem.at[0])

    zero = jnp.zeros((groups, LANES), F32)
    earlier = lax.fori_loop(0, me_t, taken, zero)
    for g in range(groups):
        entering = jnp.broadcast_to(earlier[g : g + 1], (RUNS, LANES))
        for slab in range(g * PIECES, (g + 1) * PIECES):
            for step in range(steps):
                at = pl.ds(step * PITCH, RUNS)
                own[slab, at] = own[slab, at] + through[slab, at] * entering

    for k in range(1, n_time):

        @pl.when(me_t == n_time - 1 - k)
        def _():
            arrived(inbox.at[pl.ds(0, k)], inbox_sem.at[1])

    later = lax.fori_loop(0, n_time - 1 - me_t, lambda i, state: taken(n_time - 1 - i, state), zero)

    entering = [jnp.broadcast_to(later[g : g + 1], (RUNS, LANES)) for g in range(groups)]

    def state_tile(g, row):
        run, place = divmod(row, rows // RUNS)
        piece, step = divmod(place, steps)
        slab, start = g * PIECES + piece, step * PITCH + run
        near = own[slab, pl.ds(start + RUNS, 8, stride=PITCH)]
        return own[slab, pl.ds(start, 8, stride=PITCH)] + near * entering[g]

    for b in range(rows // LANES):
        squares = []
        for row in range(b * LANES, (b + 1) * LANES, 8):
            total = None
            for g in range(groups):
                state = state_tile(g, row)
                square = state * state
                total = square if total is None else total + square
            squares.append(total)
        powers[me_c, b : b + 1] = jnp.sum(jnp.concatenate(squares, axis=0).T, axis=0, keepdims=True)

    pl.semaphore_wait(far_sem, len(around))
    for k in range(n_chan - 1):
        pltpu.make_async_remote_copy(
            src_ref=powers.at[me_c],
            dst_ref=powers.at[me_c],
            send_sem=sent_sem,
            recv_sem=power_sem,
            device_id=(me_t, k + jnp.where(k >= me_c, 1, 0)),
            device_id_type=MESH,
        ).start()
    gain_load.wait()
    for g in range(groups):
        gains = jnp.broadcast_to(gain[:, g * LANES : (g + 1) * LANES], (RUNS, LANES))
        for row in range(0, rows, 8):
            states[g, pl.ds(row, 8)] = state_tile(g, row) * gains
    arrived(powers.at[pl.ds(0, n_chan - 1)], power_sem)
    power = powers[0]
    for k in range(1, n_chan):
        power = power + powers[k]
    power_ref[...] = power

    sent = 2 * groups * (n_time - 1) + rows // LANES * (n_chan - 1)
    arrived(fade.at[0, pl.ds(0, sent)], sent_sem)


def norm_kernel(sizes, states, power, out_hbm, out, out_sem):
    channels, length = sizes
    groups, rows, _ = states.shape
    scale = lax.rsqrt(power[...] * (1.0 / channels) + 1e-06 * length)
    stores = []
    for b in range(rows // LANES):
        block = pl.ds(b * LANES, LANES)
        by_row = jnp.broadcast_to(scale[b : b + 1], (LANES, LANES)).T
        for g in range(groups):
            at = pl.ds(g * LANES, LANES)
            out[block, at] = (states[g, block] * by_row).astype(BF16)
        stores.append(pltpu.make_async_copy(out.at[block], out_hbm.at[0, block], out_sem.at[b]))
        stores[b].start()
    for store in stores:
        store.wait()


def per_device(fade_rate, update_in, norm_gain):
    n_time, n_chan = lax.axis_size("time"), lax.axis_size("chan")
    _, rows, columns = fade_rate.shape
    groups = columns // LANES
    anywhere = pl.BlockSpec(memory_space=pl.ANY)
    vmem = pl.BlockSpec(memory_space=pltpu.VMEM)
    slabs = pltpu.VMEM((PIECES * groups, rows // (PIECES * RUNS) * PITCH, LANES), F32)
    states, power = pl.pallas_call(
        functools.partial(states_kernel, (n_time, n_chan)),
        out_shape=(
            pltpu.VMEM((groups, rows, LANES), F32),
            pltpu.VMEM((rows // LANES, LANES), F32),
        ),
        in_specs=[anywhere, anywhere, anywhere],
        out_specs=(vmem, vmem),
        scratch_shapes=[
            pltpu.VMEM((groups, rows, LANES), F32),
            pltpu.VMEM((groups, rows, LANES), BF16),
            pltpu.VMEM((1, columns), F32),
            slabs,
            slabs,
            slabs,
            pltpu.VMEM((PIECES * groups, 3, RUNS, LANES), F32),
            pltpu.VMEM((groups, 3, RUNS, LANES), F32),
            pltpu.VMEM((2, 2, groups, LANES), F32),
            pltpu.VMEM((n_time, 2, groups, LANES), F32),
            pltpu.VMEM((n_chan, rows // LANES, LANES), F32),
            pltpu.SemaphoreType.DMA((groups,)),
            pltpu.SemaphoreType.DMA,
            pltpu.SemaphoreType.DMA,
            pltpu.SemaphoreType.DMA((2,)),
            pltpu.SemaphoreType.DMA,
            pltpu.SemaphoreType.REGULAR((n_time // PLANE,)),
            pltpu.SemaphoreType.REGULAR,
            pltpu.SemaphoreType.REGULAR,
            pltpu.SemaphoreType.REGULAR,
        ],
        compiler_params=pltpu.CompilerParams(collective_id=0, has_side_effects=True),
        name="filter_states",
    )(fade_rate, update_in, norm_gain.reshape(1, columns))
    states, power = (pltpu.with_memory_space_constraint(x, pltpu.VMEM) for x in (states, power))
    return pl.pallas_call(
        functools.partial(norm_kernel, (columns * n_chan, rows * n_time)),
        out_shape=jax.ShapeDtypeStruct((1, rows, columns), BF16),
        in_specs=[vmem, vmem],
        out_specs=anywhere,
        scratch_shapes=[
            pltpu.VMEM((rows, columns), BF16),
            pltpu.SemaphoreType.DMA((rows // LANES,)),
        ],
        name="channel_norm",
    )(states, power)


def solution(mesh):
    return jax.shard_map(
        per_device,
        mesh=mesh,
        in_specs=(P(None, "time", "chan"), P(None, "time", "chan"), P("chan")),
        out_specs=P(None, "time", "chan"),
        check_vma=False,
    )
```

```python
import functools

import jax
import jax.numpy as jnp
from jax import lax
from jax.experimental import pallas as pl
from jax.experimental.pallas import tpu as pltpu
from jax.sharding import PartitionSpec as P

MESH = pl.DeviceIdType.MESH
LANES = 128
RUNS = 8
PIECES = 4
PLANE = 4
CHAN_RING = 4
PITCH = 17
LOG2E = 1.4426950408889634
F32 = jnp.float32
BF16 = jnp.bfloat16


def scan_runs(weight, value, down):
    run = lax.broadcasted_iota(jnp.int32, weight.shape, 0)
    run = run if down else RUNS - 1 - run
    for gap in (1, 2, 4):
        shift = gap if down else RUNS - gap
        value = value + weight * jnp.where(run >= gap, pltpu.roll(value, shift, 0), 0.0)
        weight = weight * jnp.where(run >= gap, pltpu.roll(weight, shift, 0), 1.0)
    shift = 1 if down else RUNS - 1
    weight = jnp.where(run >= 1, pltpu.roll(weight, shift, 0), 1.0)
    return weight, jnp.where(run >= 1, pltpu.roll(value, shift, 0), 0.0)


def arrived(like, sem):
    pltpu.make_async_copy(like, like, sem).wait()


def told(sem, times):
    @pl.when(times > 0)
    def _():
        pl.semaphore_wait(sem, times)


def states_kernel(
    sizes,
    fade_hbm,
    update_hbm,
    gain_hbm,
    states,
    power_ref,
    fade,
    update,
    gain,
    flows,
    own,
    through,
    pieces,
    runs,
    message,
    inbox,
    powers,
    load_sem,
    gain_sem,
    sent_sem,
    inbox_sem,
    power_sem,
    come_sem,
    near_sem,
    middle_sem,
    far_sem,
):
    n_time, n_chan = sizes
    groups, rows, _ = fade.shape
    length = rows * n_time
    steps = rows // (RUNS * PIECES)
    for g in range(groups):
        at = pl.ds(g * LANES, LANES)
        pltpu.make_async_copy(fade_hbm.at[0, :, at], fade.at[g], load_sem.at[g]).start()
        pltpu.make_async_copy(update_hbm.at[0, :, at], update.at[g], load_sem.at[g]).start()
    gain_load = pltpu.make_async_copy(gain_hbm, gain, gain_sem)
    gain_load.start()
    pl.delay(1)

    me_t, me_c = lax.axis_index("time"), lax.axis_index("chan")
    row, cx = me_c // CHAN_RING, me_c % CHAN_RING
    around = [
        row * CHAN_RING + (cx + 1) % CHAN_RING,
        row * CHAN_RING + (cx + CHAN_RING - 1) % CHAN_RING,
        me_c + CHAN_RING - 2 * CHAN_RING * row,
    ]
    plane = me_t // PLANE
    lower_around = sum(jnp.where(peer < me_c, 1, 0) for peer in around)

    barrier = pltpu.get_barrier_semaphore()
    for peer in around:

        @pl.when(peer > me_c)
        def _():
            pl.semaphore_signal(barrier, inc=1, device_id=(me_t, peer), device_id_type=MESH)

    @pl.loop(me_t + 1, n_time)
    def _(k):
        pl.semaphore_signal(barrier, inc=1, device_id=(k, me_c), device_id_type=MESH)

    def spread(g):
        summed = None
        for i in range(0, rows, 16):
            at = pl.ds(i, 16)
            rate = fade[g, at]
            keep = jnp.exp2(rate * (-LOG2E / length))
            part = rate[:8] + rate[8:]
            summed = part if summed is None else summed + part
            push = update[g, at].astype(F32)
            for q in range(2):
                run, place = divmod(i + 8 * q, rows // RUNS)
                piece, step = divmod(place, steps)
                to = pl.ds(step * PITCH + run, 8, stride=PITCH)
                to_push = pl.ds(step * PITCH + RUNS + run, 8, stride=PITCH)
                flows[g * PIECES + piece, to] = keep[8 * q : 8 * q + 8]
                flows[g * PIECES + piece, to_push] = push[8 * q : 8 * q + 8]
        whole = jnp.exp2(jnp.sum(summed, axis=0, keepdims=True) * (-LOG2E / length))
        message[0, 0, g : g + 1] = whole
        message[1, 0, g : g + 1] = whole

    def backward_part(g):
        slabs = range(g * PIECES, (g + 1) * PIECES)
        weights = [flows[slab, pl.ds(0, RUNS)] for slab in slabs]
        behinds = [flows[slab, pl.ds(RUNS, RUNS)] for slab in slabs]
        for step in range(1, steps):
            at, at_push = pl.ds(step * PITCH, RUNS), pl.ds(step * PITCH + RUNS, RUNS)
            for p, slab in enumerate(slabs):
                behinds[p] = behinds[p] + weights[p] * flows[slab, at_push]
                weights[p] = weights[p] * flows[slab, at]
        for p, slab in enumerate(slabs):
            pieces[slab, 0], pieces[slab, 2] = weights[p], behinds[p]
        parts = list(zip(weights, behinds))
        while len(parts) > 1:
            parts = [
                (w0 * w1, b0 + w0 * b1) for (w0, b0), (w1, b1) in zip(parts[::2], parts[1::2])
            ]
        weight, behind = parts[0]
        runs[g, 0], runs[g, 2] = weight, behind
        for gap in (1, 2, 4):
            behind = behind + weight * pltpu.roll(behind, RUNS - gap, 0)
            weight = weight * pltpu.roll(weight, RUNS - gap, 0)
        message[1, 1, g : g + 1] = behind[:1]

    def forward_part(g):
        slabs = range(g * PIECES, (g + 1) * PIECES)
        aheads = [flows[slab, pl.ds(RUNS, RUNS)] for slab in slabs]
        for step in range(1, steps):
            at, at_push = pl.ds(step * PITCH, RUNS), pl.ds(step * PITCH + RUNS, RUNS)
            for p, slab in enumerate(slabs):
                aheads[p] = flows[slab, at] * aheads[p] + flows[slab, at_push]
        ahead = aheads[0]
        pieces[g * PIECES, 1] = ahead
        for p in range(1, PIECES):
            pieces[g * PIECES + p, 1] = aheads[p]
            ahead = aheads[p] + pieces[g * PIECES + p, 0] * ahead
        weight = runs[g, 0]
        runs[g, 1] = ahead
        for gap in (1, 2, 4):
            weight_next = pltpu.roll(weight, RUNS - gap, 0)
            ahead = pltpu.roll(ahead, RUNS - gap, 0) + weight_next * ahead
            weight = weight * weight_next
        message[0, 1, g : g + 1] = ahead[:1]

    for g in range(groups + 1):
        if g < groups:
            arrived(fade.at[pl.ds(0, 3), pl.ds(0, rows // 2)], load_sem.at[g])
            spread(g)
        if g > 0:
            backward_part(g - 1)

    def send_summary(k, way):
        pltpu.make_async_remote_copy(
            src_ref=message.at[way],
            dst_ref=inbox.at[me_t],
            send_sem=sent_sem,
            recv_sem=inbox_sem.at[way],
            device_id=(k, me_c),
            device_id_type=MESH,
        ).start()

    told(barrier, me_t + lower_around)
    @pl.loop(0, me_t)
    def _(k):
        send_summary(k, 1)

    for peer in around:

        @pl.when(peer < me_c)
        def _():
            pl.semaphore_signal(near_sem, inc=1, device_id=(me_t, peer), device_id_type=MESH)

    @pl.loop(0, me_t)
    def _(k):
        come = come_sem.at[plane]
        pl.semaphore_signal(come, inc=1, device_id=(k, me_c), device_id_type=MESH)

    for g in range(groups):
        forward_part(g)
    inbox[me_t] = message[0]

    told(come_sem.at[plane], PLANE - 1 - me_t % PLANE)

    @pl.loop(me_t + 1, (plane + 1) * PLANE)
    def _(k):
        send_summary(k, 0)

    def send_plane(to):
        @pl.when(to > plane)
        def _():
            pl.semaphore_wait(come_sem.at[to], PLANE)
            for k in range(to * PLANE, (to + 1) * PLANE):
                send_summary(k, 0)

    def tell_around(sem):
        for peer in around:
            pl.semaphore_signal(sem, inc=1, device_id=(me_t, peer), device_id_type=MESH)

    @pl.loop(0, groups)
    def _(g):
        slabs = [g * PIECES + p for p in range(PIECES)]
        down_in, ahead_in = scan_runs(runs[g, 0], runs[g, 1], True)
        up_in, behind_in = scan_runs(runs[g, 0], runs[g, 2], False)
        down, ahead, up, behind = [], [], [], []
        for slab in slabs:
            down.append(down_in)
            ahead.append(ahead_in)
            down_in = down_in * pieces[slab, 0]
            ahead_in = ahead_in * pieces[slab, 0] + pieces[slab, 1]
        for slab in slabs[::-1]:
            up.insert(0, up_in)
            behind.insert(0, behind_in)
            up_in = up_in * pieces[slab, 0]
            behind_in = behind_in * pieces[slab, 0] + pieces[slab, 2]
        for step in range(steps):
            at, at_2 = pl.ds(step * PITCH, RUNS), pl.ds(step * PITCH + RUNS, RUNS)
            for p, slab in enumerate(slabs):
                keep = flows[slab, at]
                ahead[p] = keep * ahead[p] + flows[slab, at_2]
                down[p] = keep * down[p]
                own[slab, at] = ahead[p]
                through[slab, at] = down[p]
        for step in range(steps - 1, -1, -1):
            at, at_2 = pl.ds(step * PITCH, RUNS), pl.ds(step * PITCH + RUNS, RUNS)
            for p, slab in enumerate(slabs):
                keep = flows[slab, at]
                behind[p] = keep * behind[p] + flows[slab, at_2]
                up[p] = keep * up[p]
                own[slab, at] = own[slab, at] + behind[p]
                own[slab, at_2] = up[p]

    told(near_sem, len(around) - lower_around)
    tell_around(middle_sem)
    for to in range(1, n_time // PLANE):
        send_plane(to)
    pl.semaphore_wait(middle_sem, len(around))
    tell_around(far_sem)

    def taken(k, state):
        return state * inbox[k, 0] + inbox[k, 1]

    for k in range(1, n_time):

        @pl.when(me_t == k)
        def _():
            arrived(inbox.at[pl.ds(0, k)], inbox_sem.at[0])

    zero = jnp.zeros((groups, LANES), F32)
    earlier = lax.fori_loop(0, me_t, taken, zero)
    for g in range(groups):
        entering = jnp.broadcast_to(earlier[g : g + 1], (RUNS, LANES))
        for slab in range(g * PIECES, (g + 1) * PIECES):
            for step in range(steps):
                at = pl.ds(step * PITCH, RUNS)
                own[slab, at] = own[slab, at] + through[slab, at] * entering

    for k in range(1, n_time):

        @pl.when(me_t == n_time - 1 - k)
        def _():
            arrived(inbox.at[pl.ds(0, k)], inbox_sem.at[1])

    later = zero
    for k in range(n_time - 1, 0, -1):
        later = jnp.where(k > me_t, taken(k, later), later)

    entering = [jnp.broadcast_to(later[g : g + 1], (RUNS, LANES)) for g in range(groups)]

    def state_tile(g, row):
        run, place = divmod(row, rows // RUNS)
        piece, step = divmod(place, steps)
        slab, start = g * PIECES + piece, step * PITCH + run
        near = own[slab, pl.ds(start + RUNS, 8, stride=PITCH)]
        return own[slab, pl.ds(start, 8, stride=PITCH)] + near * entering[g]

    for b in range(rows // LANES):
        squares = []
        for row in range(b * LANES, (b + 1) * LANES, 8):
            total = None
            for g in range(groups):
                state = state_tile(g, row)
                square = state * state
                total = square if total is None else total + square
            squares.append(total)
        powers[me_c, b : b + 1] = jnp.sum(jnp.concatenate(squares, axis=0).T, axis=0, keepdims=True)

    pl.semaphore_wait(far_sem, len(around))
    for k in range(n_chan - 1):
        pltpu.make_async_remote_copy(
            src_ref=powers.at[me_c],
            dst_ref=powers.at[me_c],
            send_sem=sent_sem,
            recv_sem=power_sem,
            device_id=(me_t, k + jnp.where(k >= me_c, 1, 0)),
            device_id_type=MESH,
        ).start()
    gain_load.wait()
    for g in range(groups):
        gains = jnp.broadcast_to(gain[:, g * LANES : (g + 1) * LANES], (RUNS, LANES))
        for row in range(0, rows, 8):
            states[g, pl.ds(row, 8)] = state_tile(g, row) * gains
    arrived(powers.at[pl.ds(0, n_chan - 1)], power_sem)
    power = powers[0]
    for k in range(1, n_chan):
        power = power + powers[k]
    power_ref[...] = power

    sent = 2 * groups * (n_time - 1) + rows // LANES * (n_chan - 1)
    arrived(fade.at[0, pl.ds(0, sent)], sent_sem)


def norm_kernel(sizes, states, power, out_hbm, out, out_sem):
    channels, length = sizes
    groups, rows, _ = states.shape
    scale = lax.rsqrt(power[...] * (1.0 / channels) + 1e-06 * length)
    stores = []
    for b in range(rows // LANES):
        block = pl.ds(b * LANES, LANES)
        by_row = jnp.broadcast_to(scale[b : b + 1], (LANES, LANES)).T
        for g in range(groups):
            at = pl.ds(g * LANES, LANES)
            out[block, at] = (states[g, block] * by_row).astype(BF16)
        stores.append(pltpu.make_async_copy(out.at[block], out_hbm.at[0, block], out_sem.at[b]))
        stores[b].start()
    for store in stores:
        store.wait()


def per_device(fade_rate, update_in, norm_gain):
    n_time, n_chan = lax.axis_size("time"), lax.axis_size("chan")
    _, rows, columns = fade_rate.shape
    groups = columns // LANES
    anywhere = pl.BlockSpec(memory_space=pl.ANY)
    vmem = pl.BlockSpec(memory_space=pltpu.VMEM)
    slabs = pltpu.VMEM((PIECES * groups, rows // (PIECES * RUNS) * PITCH, LANES), F32)
    states, power = pl.pallas_call(
        functools.partial(states_kernel, (n_time, n_chan)),
        out_shape=(
            pltpu.VMEM((groups, rows, LANES), F32),
            pltpu.VMEM((rows // LANES, LANES), F32),
        ),
        in_specs=[anywhere, anywhere, anywhere],
        out_specs=(vmem, vmem),
        scratch_shapes=[
            pltpu.VMEM((groups, rows, LANES), F32),
            pltpu.VMEM((groups, rows, LANES), BF16),
            pltpu.VMEM((1, columns), F32),
            slabs,
            slabs,
            slabs,
            pltpu.VMEM((PIECES * groups, 3, RUNS, LANES), F32),
            pltpu.VMEM((groups, 3, RUNS, LANES), F32),
            pltpu.VMEM((2, 2, groups, LANES), F32),
            pltpu.VMEM((n_time, 2, groups, LANES), F32),
            pltpu.VMEM((n_chan, rows // LANES, LANES), F32),
            pltpu.SemaphoreType.DMA((groups,)),
            pltpu.SemaphoreType.DMA,
            pltpu.SemaphoreType.DMA,
            pltpu.SemaphoreType.DMA((2,)),
            pltpu.SemaphoreType.DMA,
            pltpu.SemaphoreType.REGULAR((n_time // PLANE,)),
            pltpu.SemaphoreType.REGULAR,
            pltpu.SemaphoreType.REGULAR,
            pltpu.SemaphoreType.REGULAR,
        ],
        compiler_params=pltpu.CompilerParams(collective_id=0, has_side_effects=True),
        name="filter_states",
    )(fade_rate, update_in, norm_gain.reshape(1, columns))
    states, power = (pltpu.with_memory_space_constraint(x, pltpu.VMEM) for x in (states, power))
    return pl.pallas_call(
        functools.partial(norm_kernel, (columns * n_chan, rows * n_time)),
        out_shape=jax.ShapeDtypeStruct((1, rows, columns), BF16),
        in_specs=[vmem, vmem],
        out_specs=anywhere,
        scratch_shapes=[
            pltpu.VMEM((rows, columns), BF16),
            pltpu.SemaphoreType.DMA((rows // LANES,)),
        ],
        name="channel_norm",
    )(states, power)


def solution(mesh):
    return jax.shard_map(
        per_device,
        mesh=mesh,
        in_specs=(P(None, "time", "chan"), P(None, "time", "chan"), P("chan")),
        out_specs=P(None, "time", "chan"),
        check_vma=False,
    )
```

```python
import functools

import jax
import jax.numpy as jnp
from jax import lax
from jax.experimental import pallas as pl
from jax.experimental.pallas import tpu as pltpu
from jax.sharding import PartitionSpec as P

MESH = pl.DeviceIdType.MESH
LANES = 128
RUNS = 8
PIECES = 4
PLANE = 4
CHAN_RING = 4
PITCH = 17
LOG2E = 1.4426950408889634
F32 = jnp.float32
BF16 = jnp.bfloat16


def scan_runs(weight, value, down):
    run = lax.broadcasted_iota(jnp.int32, weight.shape, 0)
    run = run if down else RUNS - 1 - run
    for gap in (1, 2, 4):
        shift = gap if down else RUNS - gap
        value = value + weight * jnp.where(run >= gap, pltpu.roll(value, shift, 0), 0.0)
        weight = weight * jnp.where(run >= gap, pltpu.roll(weight, shift, 0), 1.0)
    shift = 1 if down else RUNS - 1
    weight = jnp.where(run >= 1, pltpu.roll(weight, shift, 0), 1.0)
    return weight, jnp.where(run >= 1, pltpu.roll(value, shift, 0), 0.0)


def arrived(like, sem):
    pltpu.make_async_copy(like, like, sem).wait()


def told(sem, times):
    @pl.when(times > 0)
    def _():
        pl.semaphore_wait(sem, times)


def states_kernel(
    sizes,
    fade_hbm,
    update_hbm,
    gain_hbm,
    states,
    power_ref,
    fade,
    update,
    gain,
    flows,
    own,
    through,
    pieces,
    runs,
    message,
    inbox,
    powers,
    load_sem,
    gain_sem,
    sent_sem,
    inbox_sem,
    power_sem,
    come_sem,
    near_sem,
    middle_sem,
    far_sem,
):
    n_time, n_chan = sizes
    groups, rows, _ = fade.shape
    length = rows * n_time
    steps = rows // (RUNS * PIECES)
    for g in range(groups):
        at = pl.ds(g * LANES, LANES)
        pltpu.make_async_copy(fade_hbm.at[0, :, at], fade.at[g], load_sem.at[g]).start()
        pltpu.make_async_copy(update_hbm.at[0, :, at], update.at[g], load_sem.at[g]).start()
    gain_load = pltpu.make_async_copy(gain_hbm, gain, gain_sem)
    gain_load.start()
    pl.delay(1)

    me_t, me_c = lax.axis_index("time"), lax.axis_index("chan")
    row, cx = me_c // CHAN_RING, me_c % CHAN_RING
    around = [
        row * CHAN_RING + (cx + 1) % CHAN_RING,
        row * CHAN_RING + (cx + CHAN_RING - 1) % CHAN_RING,
        me_c + CHAN_RING - 2 * CHAN_RING * row,
    ]
    plane = me_t // PLANE
    lower_around = sum(jnp.where(peer < me_c, 1, 0) for peer in around)

    barrier = pltpu.get_barrier_semaphore()
    for peer in around:

        @pl.when(peer > me_c)
        def _():
            pl.semaphore_signal(barrier, inc=1, device_id=(me_t, peer), device_id_type=MESH)

    @pl.loop(me_t + 1, n_time)
    def _(k):
        pl.semaphore_signal(barrier, inc=1, device_id=(k, me_c), device_id_type=MESH)

    def spread(g):
        summed = None
        for i in [run * (rows // RUNS) + p for p in range(0, rows // RUNS, 16) for run in range(RUNS)]:
            at = pl.ds(i, 16)
            rate = fade[g, at]
            keep = jnp.exp2(rate * (-LOG2E / length))
            part = rate[:8] + rate[8:]
            summed = part if summed is None else summed + part
            push = update[g, at].astype(F32)
            for q in range(2):
                run, place = divmod(i + 8 * q, rows // RUNS)
                piece, step = divmod(place, steps)
                to = pl.ds(step * PITCH + run, 8, stride=PITCH)
                to_push = pl.ds(step * PITCH + RUNS + run, 8, stride=PITCH)
                flows[g * PIECES + piece, to] = keep[8 * q : 8 * q + 8]
                flows[g * PIECES + piece, to_push] = push[8 * q : 8 * q + 8]
        whole = jnp.exp2(jnp.sum(summed, axis=0, keepdims=True) * (-LOG2E / length))
        message[0, 0, g : g + 1] = whole
        message[1, 0, g : g + 1] = whole

    def backward_part(g):
        slabs = range(g * PIECES, (g + 1) * PIECES)
        weights = [flows[slab, pl.ds(0, RUNS)] for slab in slabs]
        behinds = [flows[slab, pl.ds(RUNS, RUNS)] for slab in slabs]
        for step in range(1, steps):
            at, at_push = pl.ds(step * PITCH, RUNS), pl.ds(step * PITCH + RUNS, RUNS)
            for p, slab in enumerate(slabs):
                behinds[p] = behinds[p] + weights[p] * flows[slab, at_push]
                weights[p] = weights[p] * flows[slab, at]
        for p, slab in enumerate(slabs):
            pieces[slab, 0], pieces[slab, 2] = weights[p], behinds[p]
        parts = list(zip(weights, behinds))
        while len(parts) > 1:
            parts = [
                (w0 * w1, b0 + w0 * b1) for (w0, b0), (w1, b1) in zip(parts[::2], parts[1::2])
            ]
        weight, behind = parts[0]
        runs[g, 0], runs[g, 2] = weight, behind
        for gap in (1, 2, 4):
            behind = behind + weight * pltpu.roll(behind, RUNS - gap, 0)
            weight = weight * pltpu.roll(weight, RUNS - gap, 0)
        message[1, 1, g : g + 1] = behind[:1]

    def forward_part(g):
        slabs = range(g * PIECES, (g + 1) * PIECES)
        aheads = [flows[slab, pl.ds(RUNS, RUNS)] for slab in slabs]
        for step in range(1, steps):
            at, at_push = pl.ds(step * PITCH, RUNS), pl.ds(step * PITCH + RUNS, RUNS)
            for p, slab in enumerate(slabs):
                aheads[p] = flows[slab, at] * aheads[p] + flows[slab, at_push]
        ahead = aheads[0]
        pieces[g * PIECES, 1] = ahead
        for p in range(1, PIECES):
            pieces[g * PIECES + p, 1] = aheads[p]
            ahead = aheads[p] + pieces[g * PIECES + p, 0] * ahead
        weight = runs[g, 0]
        runs[g, 1] = ahead
        for gap in (1, 2, 4):
            weight_next = pltpu.roll(weight, RUNS - gap, 0)
            ahead = pltpu.roll(ahead, RUNS - gap, 0) + weight_next * ahead
            weight = weight * weight_next
        message[0, 1, g : g + 1] = ahead[:1]

    for g in range(groups + 1):
        if g < groups:
            arrived(fade.at[pl.ds(0, 3), pl.ds(0, rows // 2)], load_sem.at[g])
            spread(g)
        if g > 0:
            backward_part(g - 1)

    def send_summary(k, way):
        pltpu.make_async_remote_copy(
            src_ref=message.at[way],
            dst_ref=inbox.at[me_t],
            send_sem=sent_sem,
            recv_sem=inbox_sem.at[way],
            device_id=(k, me_c),
            device_id_type=MESH,
        ).start()

    told(barrier, me_t + lower_around)
    @pl.loop(0, me_t)
    def _(k):
        send_summary(k, 1)

    for peer in around:

        @pl.when(peer < me_c)
        def _():
            pl.semaphore_signal(near_sem, inc=1, device_id=(me_t, peer), device_id_type=MESH)

    @pl.loop(0, me_t)
    def _(k):
        come = come_sem.at[plane]
        pl.semaphore_signal(come, inc=1, device_id=(k, me_c), device_id_type=MESH)

    for g in range(groups):
        forward_part(g)
    inbox[me_t] = message[0]

    told(come_sem.at[plane], PLANE - 1 - me_t % PLANE)

    @pl.loop(me_t + 1, (plane + 1) * PLANE)
    def _(k):
        send_summary(k, 0)

    def send_plane(to):
        @pl.when(to > plane)
        def _():
            pl.semaphore_wait(come_sem.at[to], PLANE)
            for k in range(to * PLANE, (to + 1) * PLANE):
                send_summary(k, 0)

    def tell_around(sem):
        for peer in around:
            pl.semaphore_signal(sem, inc=1, device_id=(me_t, peer), device_id_type=MESH)

    @pl.loop(0, groups)
    def _(g):
        slabs = [g * PIECES + p for p in range(PIECES)]
        down_in, ahead_in = scan_runs(runs[g, 0], runs[g, 1], True)
        up_in, behind_in = scan_runs(runs[g, 0], runs[g, 2], False)
        down, ahead, up, behind = [], [], [], []
        for slab in slabs:
            down.append(down_in)
            ahead.append(ahead_in)
            down_in = down_in * pieces[slab, 0]
            ahead_in = ahead_in * pieces[slab, 0] + pieces[slab, 1]
        for slab in slabs[::-1]:
            up.insert(0, up_in)
            behind.insert(0, behind_in)
            up_in = up_in * pieces[slab, 0]
            behind_in = behind_in * pieces[slab, 0] + pieces[slab, 2]
        for step in range(steps):
            at, at_2 = pl.ds(step * PITCH, RUNS), pl.ds(step * PITCH + RUNS, RUNS)
            for p, slab in enumerate(slabs):
                keep = flows[slab, at]
                ahead[p] = keep * ahead[p] + flows[slab, at_2]
                down[p] = keep * down[p]
                own[slab, at] = ahead[p]
                through[slab, at] = down[p]
        for step in range(steps - 1, -1, -1):
            at, at_2 = pl.ds(step * PITCH, RUNS), pl.ds(step * PITCH + RUNS, RUNS)
            for p, slab in enumerate(slabs):
                keep = flows[slab, at]
                behind[p] = keep * behind[p] + flows[slab, at_2]
                up[p] = keep * up[p]
                own[slab, at] = own[slab, at] + behind[p]
                own[slab, at_2] = up[p]

    told(near_sem, len(around) - lower_around)
    tell_around(middle_sem)
    for to in range(1, n_time // PLANE):
        send_plane(to)
    pl.semaphore_wait(middle_sem, len(around))
    tell_around(far_sem)

    def taken(k, state):
        return state * inbox[k, 0] + inbox[k, 1]

    for k in range(1, n_time):

        @pl.when(me_t == k)
        def _():
            arrived(inbox.at[pl.ds(0, k)], inbox_sem.at[0])

    zero = jnp.zeros((groups, LANES), F32)
    earlier = lax.fori_loop(0, me_t, taken, zero)
    for g in range(groups):
        entering = jnp.broadcast_to(earlier[g : g + 1], (RUNS, LANES))
        for slab in range(g * PIECES, (g + 1) * PIECES):
            for step in range(steps):
                at = pl.ds(step * PITCH, RUNS)
                own[slab, at] = own[slab, at] + through[slab, at] * entering

    for k in range(1, n_time):

        @pl.when(me_t == n_time - 1 - k)
        def _():
            arrived(inbox.at[pl.ds(0, k)], inbox_sem.at[1])

    joined = [
        (jnp.where(k > me_t, inbox[k, 0], 1.0), jnp.where(k > me_t, inbox[k, 1], 0.0))
        for k in range(n_time - 1, 0, -1)
    ]
    while len(joined) > 1:
        joined = [
            (joined[k][0] * joined[k + 1][0], joined[k][1] * joined[k + 1][0] + joined[k + 1][1])
            for k in range(0, len(joined) - 1, 2)
        ] + joined[len(joined) // 2 * 2 :]
    later = joined[0][1]

    entering = [jnp.broadcast_to(later[g : g + 1], (RUNS, LANES)) for g in range(groups)]

    def state_tile(g, row):
        run, place = divmod(row, rows // RUNS)
        piece, step = divmod(place, steps)
        slab, start = g * PIECES + piece, step * PITCH + run
        near = own[slab, pl.ds(start + RUNS, 8, stride=PITCH)]
        return own[slab, pl.ds(start, 8, stride=PITCH)] + near * entering[g]

    for b in range(rows // LANES):
        squares = []
        for row in range(b * LANES, (b + 1) * LANES, 8):
            total = None
            for g in range(groups):
                state = state_tile(g, row)
                square = state * state
                total = square if total is None else total + square
            squares.append(total)
        powers[me_c, b : b + 1] = jnp.sum(jnp.concatenate(squares, axis=0).T, axis=0, keepdims=True)

    pl.semaphore_wait(far_sem, len(around))
    for k in range(n_chan - 1):
        pltpu.make_async_remote_copy(
            src_ref=powers.at[me_c],
            dst_ref=powers.at[me_c],
            send_sem=sent_sem,
            recv_sem=power_sem,
            device_id=(me_t, k + jnp.where(k >= me_c, 1, 0)),
            device_id_type=MESH,
        ).start()
    gain_load.wait()
    for g in range(groups):
        gains = jnp.broadcast_to(gain[:, g * LANES : (g + 1) * LANES], (RUNS, LANES))
        for row in range(0, rows, 8):
            states[g, pl.ds(row, 8)] = state_tile(g, row) * gains
    arrived(powers.at[pl.ds(0, n_chan - 1)], power_sem)
    power = powers[0]
    for k in range(1, n_chan):
        power = power + powers[k]
    power_ref[...] = power

    sent = 2 * groups * (n_time - 1) + rows // LANES * (n_chan - 1)
    arrived(fade.at[0, pl.ds(0, sent)], sent_sem)


def norm_kernel(sizes, states, power, out_hbm, out, out_sem):
    channels, length = sizes
    groups, rows, _ = states.shape
    scale = lax.rsqrt(power[...] * (1.0 / channels) + 1e-06 * length)
    stores = []
    for b in range(rows // LANES):
        block = pl.ds(b * LANES, LANES)
        by_row = jnp.broadcast_to(scale[b : b + 1], (LANES, LANES)).T
        for g in range(groups):
            at = pl.ds(g * LANES, LANES)
            out[block, at] = (states[g, block] * by_row).astype(BF16)
        stores.append(pltpu.make_async_copy(out.at[block], out_hbm.at[0, block], out_sem.at[b]))
        stores[b].start()
    for store in stores:
        store.wait()


def per_device(fade_rate, update_in, norm_gain):
    n_time, n_chan = lax.axis_size("time"), lax.axis_size("chan")
    _, rows, columns = fade_rate.shape
    groups = columns // LANES
    anywhere = pl.BlockSpec(memory_space=pl.ANY)
    vmem = pl.BlockSpec(memory_space=pltpu.VMEM)
    slabs = pltpu.VMEM((PIECES * groups, rows // (PIECES * RUNS) * PITCH, LANES), F32)
    states, power = pl.pallas_call(
        functools.partial(states_kernel, (n_time, n_chan)),
        out_shape=(
            pltpu.VMEM((groups, rows, LANES), F32),
            pltpu.VMEM((rows // LANES, LANES), F32),
        ),
        in_specs=[anywhere, anywhere, anywhere],
        out_specs=(vmem, vmem),
        scratch_shapes=[
            pltpu.VMEM((groups, rows, LANES), F32),
            pltpu.VMEM((groups, rows, LANES), BF16),
            pltpu.VMEM((1, columns), F32),
            slabs,
            slabs,
            slabs,
            pltpu.VMEM((PIECES * groups, 3, RUNS, LANES), F32),
            pltpu.VMEM((groups, 3, RUNS, LANES), F32),
            pltpu.VMEM((2, 2, groups, LANES), F32),
            pltpu.VMEM((n_time, 2, groups, LANES), F32),
            pltpu.VMEM((n_chan, rows // LANES, LANES), F32),
            pltpu.SemaphoreType.DMA((groups,)),
            pltpu.SemaphoreType.DMA,
            pltpu.SemaphoreType.DMA,
            pltpu.SemaphoreType.DMA((2,)),
            pltpu.SemaphoreType.DMA,
            pltpu.SemaphoreType.REGULAR((n_time // PLANE,)),
            pltpu.SemaphoreType.REGULAR,
            pltpu.SemaphoreType.REGULAR,
            pltpu.SemaphoreType.REGULAR,
        ],
        compiler_params=pltpu.CompilerParams(collective_id=0, has_side_effects=True),
        name="filter_states",
    )(fade_rate, update_in, norm_gain.reshape(1, columns))
    states, power = (pltpu.with_memory_space_constraint(x, pltpu.VMEM) for x in (states, power))
    return pl.pallas_call(
        functools.partial(norm_kernel, (columns * n_chan, rows * n_time)),
        out_shape=jax.ShapeDtypeStruct((1, rows, columns), BF16),
        in_specs=[vmem, vmem],
        out_specs=anywhere,
        scratch_shapes=[
            pltpu.VMEM((rows, columns), BF16),
            pltpu.SemaphoreType.DMA((rows // LANES,)),
        ],
        name="channel_norm",
    )(states, power)


def solution(mesh):
    return jax.shard_map(
        per_device,
        mesh=mesh,
        in_specs=(P(None, "time", "chan"), P(None, "time", "chan"), P("chan")),
        out_specs=P(None, "time", "chan"),
        check_vma=False,
    )
```

```python
import functools

import jax
import jax.numpy as jnp
from jax import lax
from jax.experimental import pallas as pl
from jax.experimental.pallas import tpu as pltpu
from jax.sharding import PartitionSpec as P

MESH = pl.DeviceIdType.MESH
LANES = 128
RUNS = 8
PIECES = 4
PLANE = 4
CHAN_RING = 4
PITCH = 17
LOG2E = 1.4426950408889634
F32 = jnp.float32
BF16 = jnp.bfloat16


def scan_runs(weight, value, down):
    run = lax.broadcasted_iota(jnp.int32, weight.shape, 0)
    run = run if down else RUNS - 1 - run
    for gap in (1, 2, 4):
        shift = gap if down else RUNS - gap
        value = value + weight * jnp.where(run >= gap, pltpu.roll(value, shift, 0), 0.0)
        weight = weight * jnp.where(run >= gap, pltpu.roll(weight, shift, 0), 1.0)
    shift = 1 if down else RUNS - 1
    weight = jnp.where(run >= 1, pltpu.roll(weight, shift, 0), 1.0)
    return weight, jnp.where(run >= 1, pltpu.roll(value, shift, 0), 0.0)


def arrived(like, sem):
    pltpu.make_async_copy(like, like, sem).wait()


def told(sem, times):
    @pl.when(times > 0)
    def _():
        pl.semaphore_wait(sem, times)


def states_kernel(
    sizes,
    fade_hbm,
    update_hbm,
    gain_hbm,
    states,
    power_ref,
    fade,
    update,
    gain,
    flows,
    own,
    through,
    pieces,
    runs,
    message,
    inbox,
    powers,
    sent_sem,
    inbox_sem,
    power_sem,
    come_sem,
    near_sem,
    middle_sem,
    far_sem,
):
    n_time, n_chan = sizes
    groups, rows, _ = fade.shape
    length = rows * n_time
    steps = rows // (RUNS * PIECES)
    def places():
        me_t, me_c = lax.axis_index("time"), lax.axis_index("chan")
        row, cx = me_c // CHAN_RING, me_c % CHAN_RING
        around = [
            row * CHAN_RING + (cx + 1) % CHAN_RING,
            row * CHAN_RING + (cx + CHAN_RING - 1) % CHAN_RING,
            me_c + CHAN_RING - 2 * CHAN_RING * row,
        ]
        plane = me_t // PLANE
        lower_around = sum(jnp.where(peer < me_c, 1, 0) for peer in around)
        return me_t, me_c, plane, around, lower_around

    barrier = pltpu.get_barrier_semaphore()

    def spread(g):
        summed = None
        for i in [run * (rows // RUNS) + p for p in range(0, rows // RUNS, 16) for run in range(RUNS)]:
            at = pl.ds(i, 16)
            rate = fade[g, at]
            keep = jnp.exp2(rate * (-LOG2E / length))
            part = rate[:8] + rate[8:]
            summed = part if summed is None else summed + part
            push = update[g, at].astype(F32)
            for q in range(2):
                run, place = divmod(i + 8 * q, rows // RUNS)
                piece, step = divmod(place, steps)
                to = pl.ds(step * PITCH + run, 8, stride=PITCH)
                to_push = pl.ds(step * PITCH + RUNS + run, 8, stride=PITCH)
                flows[g * PIECES + piece, to] = keep[8 * q : 8 * q + 8]
                flows[g * PIECES + piece, to_push] = push[8 * q : 8 * q + 8]
        whole = jnp.exp2(jnp.sum(summed, axis=0, keepdims=True) * (-LOG2E / length))
        message[0, 0, g : g + 1] = whole
        message[1, 0, g : g + 1] = whole

    def backward_part(g):
        slabs = range(g * PIECES, (g + 1) * PIECES)
        weights = [flows[slab, pl.ds(0, RUNS)] for slab in slabs]
        behinds = [flows[slab, pl.ds(RUNS, RUNS)] for slab in slabs]
        for step in range(1, steps):
            at, at_push = pl.ds(step * PITCH, RUNS), pl.ds(step * PITCH + RUNS, RUNS)
            for p, slab in enumerate(slabs):
                behinds[p] = behinds[p] + weights[p] * flows[slab, at_push]
                weights[p] = weights[p] * flows[slab, at]
        for p, slab in enumerate(slabs):
            pieces[slab, 0], pieces[slab, 2] = weights[p], behinds[p]
        parts = list(zip(weights, behinds))
        while len(parts) > 1:
            parts = [
                (w0 * w1, b0 + w0 * b1) for (w0, b0), (w1, b1) in zip(parts[::2], parts[1::2])
            ]
        weight, behind = parts[0]
        runs[g, 0], runs[g, 2] = weight, behind
        for gap in (1, 2, 4):
            behind = behind + weight * pltpu.roll(behind, RUNS - gap, 0)
            weight = weight * pltpu.roll(weight, RUNS - gap, 0)
        message[1, 1, g : g + 1] = behind[:1]

    def forward_part(g):
        slabs = range(g * PIECES, (g + 1) * PIECES)
        aheads = [flows[slab, pl.ds(RUNS, RUNS)] for slab in slabs]
        for step in range(1, steps):
            at, at_push = pl.ds(step * PITCH, RUNS), pl.ds(step * PITCH + RUNS, RUNS)
            for p, slab in enumerate(slabs):
                aheads[p] = flows[slab, at] * aheads[p] + flows[slab, at_push]
        ahead = aheads[0]
        pieces[g * PIECES, 1] = ahead
        for p in range(1, PIECES):
            pieces[g * PIECES + p, 1] = aheads[p]
            ahead = aheads[p] + pieces[g * PIECES + p, 0] * ahead
        weight = runs[g, 0]
        runs[g, 1] = ahead
        for gap in (1, 2, 4):
            weight_next = pltpu.roll(weight, RUNS - gap, 0)
            ahead = pltpu.roll(ahead, RUNS - gap, 0) + weight_next * ahead
            weight = weight * weight_next
        message[0, 1, g : g + 1] = ahead[:1]

    def send_summary(me_t, me_c, k, way):
        pltpu.make_async_remote_copy(
            src_ref=message.at[way],
            dst_ref=inbox.at[me_t],
            send_sem=sent_sem,
            recv_sem=inbox_sem.at[way],
            device_id=(k, me_c),
            device_id_type=MESH,
        ).start()

    def load_and_send(load_sem, gain_sem):
        for g in range(groups):
            at = pl.ds(g * LANES, LANES)
            pltpu.make_async_copy(fade_hbm.at[0, :, at], fade.at[g], load_sem.at[g]).start()
            pltpu.make_async_copy(update_hbm.at[0, :, at], update.at[g], load_sem.at[g]).start()
        gain_load = pltpu.make_async_copy(gain_hbm, gain, gain_sem)
        gain_load.start()
        pl.delay(1)
        me_t, me_c, plane, around, lower_around = places()

        for peer in around:

            @pl.when(peer > me_c)
            def _():
                pl.semaphore_signal(barrier, inc=1, device_id=(me_t, peer), device_id_type=MESH)

        @pl.loop(me_t + 1, n_time)
        def _(k):
            pl.semaphore_signal(barrier, inc=1, device_id=(k, me_c), device_id_type=MESH)

        for g in range(groups + 1):
            if g < groups:
                arrived(fade.at[pl.ds(0, 3), pl.ds(0, rows // 2)], load_sem.at[g])
                spread(g)
            if g > 0:
                backward_part(g - 1)

        told(barrier, me_t + lower_around)

        @pl.loop(0, me_t)
        def _(k):
            send_summary(me_t, me_c, k, 1)

        for peer in around:

            @pl.when(peer < me_c)
            def _():
                pl.semaphore_signal(near_sem, inc=1, device_id=(me_t, peer), device_id_type=MESH)

        @pl.loop(0, me_t)
        def _(k):
            come = come_sem.at[plane]
            pl.semaphore_signal(come, inc=1, device_id=(k, me_c), device_id_type=MESH)

        gain_load.wait()

    pl.run_scoped(load_and_send, pltpu.SemaphoreType.DMA((groups,)), pltpu.SemaphoreType.DMA)

    me_t, me_c, plane, around, lower_around = places()

    for g in range(groups):
        forward_part(g)
    inbox[me_t] = message[0]

    told(come_sem.at[plane], PLANE - 1 - me_t % PLANE)

    @pl.loop(me_t + 1, (plane + 1) * PLANE)
    def _(k):
        send_summary(me_t, me_c, k, 0)

    def send_plane(to):
        @pl.when(to > plane)
        def _():
            pl.semaphore_wait(come_sem.at[to], PLANE)
            for k in range(to * PLANE, (to + 1) * PLANE):
                send_summary(me_t, me_c, k, 0)

    def tell_around(sem):
        for peer in around:
            pl.semaphore_signal(sem, inc=1, device_id=(me_t, peer), device_id_type=MESH)

    @pl.loop(0, groups)
    def _(g):
        slabs = [g * PIECES + p for p in range(PIECES)]
        down_in, ahead_in = scan_runs(runs[g, 0], runs[g, 1], True)
        up_in, behind_in = scan_runs(runs[g, 0], runs[g, 2], False)
        down, ahead, up, behind = [], [], [], []
        for slab in slabs:
            down.append(down_in)
            ahead.append(ahead_in)
            down_in = down_in * pieces[slab, 0]
            ahead_in = ahead_in * pieces[slab, 0] + pieces[slab, 1]
        for slab in slabs[::-1]:
            up.insert(0, up_in)
            behind.insert(0, behind_in)
            up_in = up_in * pieces[slab, 0]
            behind_in = behind_in * pieces[slab, 0] + pieces[slab, 2]
        for step in range(steps):
            at, at_2 = pl.ds(step * PITCH, RUNS), pl.ds(step * PITCH + RUNS, RUNS)
            for p, slab in enumerate(slabs):
                keep = flows[slab, at]
                ahead[p] = keep * ahead[p] + flows[slab, at_2]
                down[p] = keep * down[p]
                own[slab, at] = ahead[p]
                through[slab, at] = down[p]
        for step in range(steps - 1, -1, -1):
            at, at_2 = pl.ds(step * PITCH, RUNS), pl.ds(step * PITCH + RUNS, RUNS)
            for p, slab in enumerate(slabs):
                keep = flows[slab, at]
                behind[p] = keep * behind[p] + flows[slab, at_2]
                up[p] = keep * up[p]
                own[slab, at] = own[slab, at] + behind[p]
                own[slab, at_2] = up[p]

    told(near_sem, len(around) - lower_around)
    tell_around(middle_sem)
    for to in range(1, n_time // PLANE):
        send_plane(to)
    pl.semaphore_wait(middle_sem, len(around))
    tell_around(far_sem)

    def taken(k, state):
        return state * inbox[k, 0] + inbox[k, 1]

    for k in range(1, n_time):

        @pl.when(me_t == k)
        def _():
            arrived(inbox.at[pl.ds(0, k)], inbox_sem.at[0])

    zero = jnp.zeros((groups, LANES), F32)
    earlier = lax.fori_loop(0, me_t, taken, zero)
    for g in range(groups):
        entering = jnp.broadcast_to(earlier[g : g + 1], (RUNS, LANES))
        for slab in range(g * PIECES, (g + 1) * PIECES):
            for step in range(steps):
                at = pl.ds(step * PITCH, RUNS)
                own[slab, at] = own[slab, at] + through[slab, at] * entering

    for k in range(1, n_time):

        @pl.when(me_t == n_time - 1 - k)
        def _():
            arrived(inbox.at[pl.ds(0, k)], inbox_sem.at[1])

    joined = [
        (jnp.where(k > me_t, inbox[k, 0], 1.0), jnp.where(k > me_t, inbox[k, 1], 0.0))
        for k in range(n_time - 1, 0, -1)
    ]
    while len(joined) > 1:
        joined = [
            (joined[k][0] * joined[k + 1][0], joined[k][1] * joined[k + 1][0] + joined[k + 1][1])
            for k in range(0, len(joined) - 1, 2)
        ] + joined[len(joined) // 2 * 2 :]
    later = joined[0][1]

    entering = [jnp.broadcast_to(later[g : g + 1], (RUNS, LANES)) for g in range(groups)]

    def state_tile(g, row):
        run, place = divmod(row, rows // RUNS)
        piece, step = divmod(place, steps)
        slab, start = g * PIECES + piece, step * PITCH + run
        near = own[slab, pl.ds(start + RUNS, 8, stride=PITCH)]
        return own[slab, pl.ds(start, 8, stride=PITCH)] + near * entering[g]

    for b in range(rows // LANES):
        squares = []
        for row in range(b * LANES, (b + 1) * LANES, 8):
            total = None
            for g in range(groups):
                state = state_tile(g, row)
                square = state * state
                total = square if total is None else total + square
            squares.append(total)
        powers[me_c, b : b + 1] = jnp.sum(jnp.concatenate(squares, axis=0).T, axis=0, keepdims=True)

    pl.semaphore_wait(far_sem, len(around))
    for k in range(n_chan - 1):
        pltpu.make_async_remote_copy(
            src_ref=powers.at[me_c],
            dst_ref=powers.at[me_c],
            send_sem=sent_sem,
            recv_sem=power_sem,
            device_id=(me_t, k + jnp.where(k >= me_c, 1, 0)),
            device_id_type=MESH,
        ).start()
    for g in range(groups):
        gains = jnp.broadcast_to(gain[:, g * LANES : (g + 1) * LANES], (RUNS, LANES))
        for row in range(0, rows, 8):
            states[g, pl.ds(row, 8)] = state_tile(g, row) * gains
    arrived(powers.at[pl.ds(0, n_chan - 1)], power_sem)
    power = powers[0]
    for k in range(1, n_chan):
        power = power + powers[k]
    power_ref[...] = power

    sent = 2 * groups * (n_time - 1) + rows // LANES * (n_chan - 1)
    arrived(fade.at[0, pl.ds(0, sent)], sent_sem)


def norm_kernel(sizes, states, power, out_hbm, out, out_sem):
    channels, length = sizes
    groups, rows, _ = states.shape
    scale = lax.rsqrt(power[...] * (1.0 / channels) + 1e-06 * length)
    for b in range(rows // LANES):
        block = pl.ds(b * LANES, LANES)
        by_row = jnp.broadcast_to(scale[b : b + 1], (LANES, LANES)).T
        for g in range(groups):
            at = pl.ds(g * LANES, LANES)
            out[block, at] = (states[g, block] * by_row).astype(BF16)
        pltpu.make_async_copy(out.at[block], out_hbm.at[0, block], out_sem).start()
    arrived(out, out_sem)


def per_device(fade_rate, update_in, norm_gain):
    n_time, n_chan = lax.axis_size("time"), lax.axis_size("chan")
    _, rows, columns = fade_rate.shape
    groups = columns // LANES
    anywhere = pl.BlockSpec(memory_space=pl.ANY)
    vmem = pl.BlockSpec(memory_space=pltpu.VMEM)
    slabs = pltpu.VMEM((PIECES * groups, rows // (PIECES * RUNS) * PITCH, LANES), F32)
    states, power = pl.pallas_call(
        functools.partial(states_kernel, (n_time, n_chan)),
        out_shape=(
            pltpu.VMEM((groups, rows, LANES), F32),
            pltpu.VMEM((rows // LANES, LANES), F32),
        ),
        in_specs=[anywhere, anywhere, anywhere],
        out_specs=(vmem, vmem),
        scratch_shapes=[
            pltpu.VMEM((groups, rows, LANES), F32),
            pltpu.VMEM((groups, rows, LANES), BF16),
            pltpu.VMEM((1, columns), F32),
            slabs,
            slabs,
            slabs,
            pltpu.VMEM((PIECES * groups, 3, RUNS, LANES), F32),
            pltpu.VMEM((groups, 3, RUNS, LANES), F32),
            pltpu.VMEM((2, 2, groups, LANES), F32),
            pltpu.VMEM((n_time, 2, groups, LANES), F32),
            pltpu.VMEM((n_chan, rows // LANES, LANES), F32),
            pltpu.SemaphoreType.DMA,
            pltpu.SemaphoreType.DMA((2,)),
            pltpu.SemaphoreType.DMA,
            pltpu.SemaphoreType.REGULAR((n_time // PLANE,)),
            pltpu.SemaphoreType.REGULAR,
            pltpu.SemaphoreType.REGULAR,
            pltpu.SemaphoreType.REGULAR,
        ],
        compiler_params=pltpu.CompilerParams(collective_id=0, has_side_effects=True),
        name="filter_states",
    )(fade_rate, update_in, norm_gain.reshape(1, columns))
    states, power = (pltpu.with_memory_space_constraint(x, pltpu.VMEM) for x in (states, power))
    return pl.pallas_call(
        functools.partial(norm_kernel, (columns * n_chan, rows * n_time)),
        out_shape=jax.ShapeDtypeStruct((1, rows, columns), BF16),
        in_specs=[vmem, vmem],
        out_specs=anywhere,
        scratch_shapes=[
            pltpu.VMEM((rows, columns), BF16),
            pltpu.SemaphoreType.DMA,
        ],
        name="channel_norm",
    )(states, power)


def solution(mesh):
    return jax.shard_map(
        per_device,
        mesh=mesh,
        in_specs=(P(None, "time", "chan"), P(None, "time", "chan"), P("chan")),
        out_specs=P(None, "time", "chan"),
        check_vma=False,
    )
```

```python
import functools

import jax
import jax.numpy as jnp
from jax import lax
from jax.experimental import pallas as pl
from jax.experimental.pallas import tpu as pltpu
from jax.sharding import PartitionSpec as P

MESH = pl.DeviceIdType.MESH
LANES = 128
RUNS = 8
PIECES = 4
PLANE = 4
CHAN_RING = 4
PITCH = 17
LOG2E = 1.4426950408889634
F32 = jnp.float32
BF16 = jnp.bfloat16


def scan_runs(weight, value, down):
    run = lax.broadcasted_iota(jnp.int32, weight.shape, 0)
    run = run if down else RUNS - 1 - run
    for gap in (1, 2, 4):
        shift = gap if down else RUNS - gap
        value = value + weight * jnp.where(run >= gap, pltpu.roll(value, shift, 0), 0.0)
        weight = weight * jnp.where(run >= gap, pltpu.roll(weight, shift, 0), 1.0)
    shift = 1 if down else RUNS - 1
    weight = jnp.where(run >= 1, pltpu.roll(weight, shift, 0), 1.0)
    return weight, jnp.where(run >= 1, pltpu.roll(value, shift, 0), 0.0)


def arrived(like, sem):
    pltpu.make_async_copy(like, like, sem).wait()


def told(sem, times):
    @pl.when(times > 0)
    def _():
        pl.semaphore_wait(sem, times)


def states_kernel(
    sizes,
    fade_hbm,
    update_hbm,
    gain_hbm,
    states,
    power_ref,
    fade,
    update,
    gain,
    flows,
    own,
    through,
    pieces,
    runs,
    message,
    inbox,
    powers,
    sent_sem,
    inbox_sem,
    power_sem,
    come_sem,
    near_sem,
    middle_sem,
    far_sem,
):
    n_time, n_chan = sizes
    groups, rows, _ = fade.shape
    length = rows * n_time
    steps = rows // (RUNS * PIECES)
    def places():
        me_t, me_c = lax.axis_index("time"), lax.axis_index("chan")
        row, cx = me_c // CHAN_RING, me_c % CHAN_RING
        around = [
            row * CHAN_RING + (cx + 1) % CHAN_RING,
            row * CHAN_RING + (cx + CHAN_RING - 1) % CHAN_RING,
            me_c + CHAN_RING - 2 * CHAN_RING * row,
        ]
        plane = me_t // PLANE
        lower_around = sum(jnp.where(peer < me_c, 1, 0) for peer in around)
        return me_t, me_c, plane, around, lower_around

    barrier = pltpu.get_barrier_semaphore()

    def spread(g):
        summed = None
        for i in [run * (rows // RUNS) + p for p in range(0, rows // RUNS, 16) for run in range(RUNS)]:
            at = pl.ds(i, 16)
            rate = fade[g, at]
            keep = jnp.exp2(rate * (-LOG2E / length))
            part = rate[:8] + rate[8:]
            summed = part if summed is None else summed + part
            push = update[g, at].astype(F32)
            for q in range(2):
                run, place = divmod(i + 8 * q, rows // RUNS)
                piece, step = divmod(place, steps)
                to = pl.ds(step * PITCH + run, 8, stride=PITCH)
                to_push = pl.ds(step * PITCH + RUNS + run, 8, stride=PITCH)
                flows[g * PIECES + piece, to] = keep[8 * q : 8 * q + 8]
                flows[g * PIECES + piece, to_push] = push[8 * q : 8 * q + 8]
        whole = jnp.exp2(jnp.sum(summed, axis=0, keepdims=True) * (-LOG2E / length))
        message[0, 0, g : g + 1] = whole
        message[1, 0, g : g + 1] = whole

    def backward_part(g):
        slabs = range(g * PIECES, (g + 1) * PIECES)
        weights = [flows[slab, pl.ds(0, RUNS)] for slab in slabs]
        behinds = [flows[slab, pl.ds(RUNS, RUNS)] for slab in slabs]
        for step in range(1, steps):
            at, at_push = pl.ds(step * PITCH, RUNS), pl.ds(step * PITCH + RUNS, RUNS)
            for p, slab in enumerate(slabs):
                behinds[p] = behinds[p] + weights[p] * flows[slab, at_push]
                weights[p] = weights[p] * flows[slab, at]
        for p, slab in enumerate(slabs):
            pieces[slab, 0], pieces[slab, 2] = weights[p], behinds[p]
        parts = list(zip(weights, behinds))
        while len(parts) > 1:
            parts = [
                (w0 * w1, b0 + w0 * b1) for (w0, b0), (w1, b1) in zip(parts[::2], parts[1::2])
            ]
        weight, behind = parts[0]
        runs[g, 0], runs[g, 2] = weight, behind
        for gap in (1, 2, 4):
            behind = behind + weight * pltpu.roll(behind, RUNS - gap, 0)
            weight = weight * pltpu.roll(weight, RUNS - gap, 0)
        message[1, 1, g : g + 1] = behind[:1]

    def forward_part(g):
        slabs = range(g * PIECES, (g + 1) * PIECES)
        aheads = [flows[slab, pl.ds(RUNS, RUNS)] for slab in slabs]
        for step in range(1, steps):
            at, at_push = pl.ds(step * PITCH, RUNS), pl.ds(step * PITCH + RUNS, RUNS)
            for p, slab in enumerate(slabs):
                aheads[p] = flows[slab, at] * aheads[p] + flows[slab, at_push]
        ahead = aheads[0]
        pieces[g * PIECES, 1] = ahead
        for p in range(1, PIECES):
            pieces[g * PIECES + p, 1] = aheads[p]
            ahead = aheads[p] + pieces[g * PIECES + p, 0] * ahead
        weight = runs[g, 0]
        runs[g, 1] = ahead
        for gap in (1, 2, 4):
            weight_next = pltpu.roll(weight, RUNS - gap, 0)
            ahead = pltpu.roll(ahead, RUNS - gap, 0) + weight_next * ahead
            weight = weight * weight_next
        message[0, 1, g : g + 1] = ahead[:1]

    def send_summary(me_t, me_c, k, way):
        pltpu.make_async_remote_copy(
            src_ref=message.at[way],
            dst_ref=inbox.at[me_t],
            send_sem=sent_sem,
            recv_sem=inbox_sem.at[way],
            device_id=(k, me_c),
            device_id_type=MESH,
        ).start()

    def load_and_send(load_sem, gain_sem):
        for g in range(groups):
            at = pl.ds(g * LANES, LANES)
            pltpu.make_async_copy(fade_hbm.at[0, :, at], fade.at[g], load_sem.at[g]).start()
            pltpu.make_async_copy(update_hbm.at[0, :, at], update.at[g], load_sem.at[g]).start()
        gain_load = pltpu.make_async_copy(gain_hbm, gain, gain_sem)
        gain_load.start()
        pl.delay(1)
        me_t, me_c, plane, around, lower_around = places()

        for peer in around:

            @pl.when(peer > me_c)
            def _():
                pl.semaphore_signal(barrier, inc=1, device_id=(me_t, peer), device_id_type=MESH)

        @pl.loop(me_t + 1, n_time)
        def _(k):
            pl.semaphore_signal(barrier, inc=1, device_id=(k, me_c), device_id_type=MESH)

        for g in range(groups + 1):
            if g < groups:
                arrived(fade.at[pl.ds(0, 3), pl.ds(0, rows // 2)], load_sem.at[g])
                spread(g)
            if g > 0:
                backward_part(g - 1)

        told(barrier, me_t + lower_around)

        @pl.loop(0, me_t)
        def _(k):
            send_summary(me_t, me_c, k, 1)

        for peer in around:

            @pl.when(peer < me_c)
            def _():
                pl.semaphore_signal(near_sem, inc=1, device_id=(me_t, peer), device_id_type=MESH)

        @pl.loop(0, me_t)
        def _(k):
            come = come_sem.at[plane]
            pl.semaphore_signal(come, inc=1, device_id=(k, me_c), device_id_type=MESH)

        gain_load.wait()

    pl.run_scoped(load_and_send, pltpu.SemaphoreType.DMA((groups,)), pltpu.SemaphoreType.DMA)

    me_t, me_c, plane, around, lower_around = places()

    for g in range(groups):
        forward_part(g)
    inbox[me_t] = message[0]

    told(come_sem.at[plane], PLANE - 1 - me_t % PLANE)

    @pl.loop(me_t + 1, (plane + 1) * PLANE)
    def _(k):
        send_summary(me_t, me_c, k, 0)

    def send_plane(to):
        @pl.when(to > plane)
        def _():
            pl.semaphore_wait(come_sem.at[to], PLANE)
            for k in range(to * PLANE, (to + 1) * PLANE):
                send_summary(me_t, me_c, k, 0)

    def tell_around(sem):
        for peer in around:
            pl.semaphore_signal(sem, inc=1, device_id=(me_t, peer), device_id_type=MESH)

    @pl.loop(0, groups)
    def _(g):
        slabs = [g * PIECES + p for p in range(PIECES)]
        down_in, ahead_in = scan_runs(runs[g, 0], runs[g, 1], True)
        up_in, behind_in = scan_runs(runs[g, 0], runs[g, 2], False)
        down, ahead, up, behind = [], [], [], []
        for slab in slabs:
            down.append(down_in)
            ahead.append(ahead_in)
            down_in = down_in * pieces[slab, 0]
            ahead_in = ahead_in * pieces[slab, 0] + pieces[slab, 1]
        for slab in slabs[::-1]:
            up.insert(0, up_in)
            behind.insert(0, behind_in)
            up_in = up_in * pieces[slab, 0]
            behind_in = behind_in * pieces[slab, 0] + pieces[slab, 2]
        for step in range(steps):
            at, at_2 = pl.ds(step * PITCH, RUNS), pl.ds(step * PITCH + RUNS, RUNS)
            for p, slab in enumerate(slabs):
                keep = flows[slab, at]
                ahead[p] = keep * ahead[p] + flows[slab, at_2]
                down[p] = keep * down[p]
                own[slab, at] = ahead[p]
                through[slab, at] = down[p]
        for step in range(steps - 1, -1, -1):
            at, at_2 = pl.ds(step * PITCH, RUNS), pl.ds(step * PITCH + RUNS, RUNS)
            for p, slab in enumerate(slabs):
                keep = flows[slab, at]
                behind[p] = keep * behind[p] + flows[slab, at_2]
                up[p] = keep * up[p]
                own[slab, at] = own[slab, at] + behind[p]
                own[slab, at_2] = up[p]

    told(near_sem, len(around) - lower_around)
    tell_around(middle_sem)
    for to in range(1, n_time // PLANE):
        send_plane(to)
    pl.semaphore_wait(middle_sem, len(around))
    tell_around(far_sem)

    def taken(k, state):
        return state * inbox[k, 0] + inbox[k, 1]

    for k in range(1, n_time):

        @pl.when(me_t == k)
        def _():
            arrived(inbox.at[pl.ds(0, k)], inbox_sem.at[0])

    zero = jnp.zeros((groups, LANES), F32)
    earlier = lax.fori_loop(0, me_t, taken, zero)
    for g in range(groups):
        entering = jnp.broadcast_to(earlier[g : g + 1], (RUNS, LANES))
        for slab in range(g * PIECES, (g + 1) * PIECES):
            for step in range(steps):
                at = pl.ds(step * PITCH, RUNS)
                own[slab, at] = own[slab, at] + through[slab, at] * entering

    for k in range(1, n_time):

        @pl.when(me_t == n_time - 1 - k)
        def _():
            arrived(inbox.at[pl.ds(0, k)], inbox_sem.at[1])

    joined = [
        (jnp.where(k > me_t, inbox[k, 0], 1.0), jnp.where(k > me_t, inbox[k, 1], 0.0))
        for k in range(n_time - 1, 0, -1)
    ]
    while len(joined) > 1:
        joined = [
            (joined[k][0] * joined[k + 1][0], joined[k][1] * joined[k + 1][0] + joined[k + 1][1])
            for k in range(0, len(joined) - 1, 2)
        ] + joined[len(joined) // 2 * 2 :]
    later = joined[0][1]

    entering = [jnp.broadcast_to(later[g : g + 1], (RUNS, LANES)) for g in range(groups)]

    def state_tile(g, row):
        run, place = divmod(row, rows // RUNS)
        piece, step = divmod(place, steps)
        slab, start = g * PIECES + piece, step * PITCH + run
        near = own[slab, pl.ds(start + RUNS, 8, stride=PITCH)]
        return own[slab, pl.ds(start, 8, stride=PITCH)] + near * entering[g]

    for b in range(rows // LANES):
        squares = []
        for row in range(b * LANES, (b + 1) * LANES, 8):
            total = None
            for g in range(groups):
                state = state_tile(g, row)
                square = state * state
                total = square if total is None else total + square
            squares.append(total)
        powers[me_c, b : b + 1] = jnp.sum(jnp.concatenate(squares, axis=0).T, axis=0, keepdims=True)

    pl.semaphore_wait(far_sem, len(around))
    for k in range(n_chan - 1):
        pltpu.make_async_remote_copy(
            src_ref=powers.at[me_c],
            dst_ref=powers.at[me_c],
            send_sem=sent_sem,
            recv_sem=power_sem,
            device_id=(me_t, k + jnp.where(k >= me_c, 1, 0)),
            device_id_type=MESH,
        ).start()
    for g in range(groups):
        gains = jnp.broadcast_to(gain[:, g * LANES : (g + 1) * LANES], (RUNS, LANES))
        for row in range(0, rows, 8):
            states[g, pl.ds(row, 8)] = state_tile(g, row) * gains
    arrived(powers.at[pl.ds(0, n_chan - 1)], power_sem)
    power = powers[0]
    for k in range(1, n_chan):
        power = power + powers[k]
    power_ref[...] = power

    sent = 2 * groups * (n_time - 1) + rows // LANES * (n_chan - 1)
    arrived(fade.at[0, pl.ds(0, sent)], sent_sem)


def norm_kernel(sizes, states, power, out_hbm, out, out_sem):
    channels, length = sizes
    groups, rows, _ = states.shape
    scale = lax.rsqrt(power[...] * (1.0 / channels) + 1e-06 * length)
    for b in range(rows // LANES):
        block = pl.ds(b * LANES, LANES)
        by_row = jnp.broadcast_to(scale[b : b + 1], (LANES, LANES)).T
        for g in range(groups):
            at = pl.ds(g * LANES, LANES)
            out[block, at] = (states[g, block] * by_row).astype(BF16)
        pltpu.make_async_copy(out.at[block], out_hbm.at[0, block], out_sem).start()
    arrived(out, out_sem)


def per_device(fade_rate, update_in, norm_gain):
    n_time, n_chan = lax.axis_size("time"), lax.axis_size("chan")
    _, rows, columns = fade_rate.shape
    groups = columns // LANES
    anywhere = pl.BlockSpec(memory_space=pl.ANY)
    vmem = pl.BlockSpec(memory_space=pltpu.VMEM)
    slabs = pltpu.VMEM((PIECES * groups, rows // (PIECES * RUNS) * PITCH + 32, LANES), F32)
    states, power = pl.pallas_call(
        functools.partial(states_kernel, (n_time, n_chan)),
        out_shape=(
            pltpu.VMEM((groups, rows, LANES), F32),
            pltpu.VMEM((rows // LANES, LANES), F32),
        ),
        in_specs=[anywhere, anywhere, anywhere],
        out_specs=(vmem, vmem),
        scratch_shapes=[
            pltpu.VMEM((groups, rows, LANES), F32),
            pltpu.VMEM((groups, rows, LANES), BF16),
            pltpu.VMEM((1, columns), F32),
            slabs,
            slabs,
            slabs,
            pltpu.VMEM((PIECES * groups, 3, RUNS, LANES), F32),
            pltpu.VMEM((groups, 3, RUNS, LANES), F32),
            pltpu.VMEM((2, 2, groups, LANES), F32),
            pltpu.VMEM((n_time, 2, groups, LANES), F32),
            pltpu.VMEM((n_chan, rows // LANES, LANES), F32),
            pltpu.SemaphoreType.DMA,
            pltpu.SemaphoreType.DMA((2,)),
            pltpu.SemaphoreType.DMA,
            pltpu.SemaphoreType.REGULAR((n_time // PLANE,)),
            pltpu.SemaphoreType.REGULAR,
            pltpu.SemaphoreType.REGULAR,
            pltpu.SemaphoreType.REGULAR,
        ],
        compiler_params=pltpu.CompilerParams(collective_id=0, has_side_effects=True),
        name="filter_states",
    )(fade_rate, update_in, norm_gain.reshape(1, columns))
    states, power = (pltpu.with_memory_space_constraint(x, pltpu.VMEM) for x in (states, power))
    return pl.pallas_call(
        functools.partial(norm_kernel, (columns * n_chan, rows * n_time)),
        out_shape=jax.ShapeDtypeStruct((1, rows, columns), BF16),
        in_specs=[vmem, vmem],
        out_specs=anywhere,
        scratch_shapes=[
            pltpu.VMEM((rows, columns), BF16),
            pltpu.SemaphoreType.DMA,
        ],
        name="channel_norm",
    )(states, power)


def solution(mesh):
    return jax.shard_map(
        per_device,
        mesh=mesh,
        in_specs=(P(None, "time", "chan"), P(None, "time", "chan"), P("chan")),
        out_specs=P(None, "time", "chan"),
        check_vma=False,
    )
```

```python
import functools

import jax
import jax.numpy as jnp
from jax import lax
from jax.experimental import pallas as pl
from jax.experimental.pallas import tpu as pltpu
from jax.sharding import PartitionSpec as P

MESH = pl.DeviceIdType.MESH
LANES = 128
RUNS = 8
PIECES = 4
PLANE = 4
CHAN_RING = 4
PITCH = 17
LOG2E = 1.4426950408889634
F32 = jnp.float32
BF16 = jnp.bfloat16


def scan_runs(weight, value, down):
    run = lax.broadcasted_iota(jnp.int32, weight.shape, 0)
    run = run if down else RUNS - 1 - run
    for gap in (1, 2, 4):
        shift = gap if down else RUNS - gap
        value = value + weight * jnp.where(run >= gap, pltpu.roll(value, shift, 0), 0.0)
        weight = weight * jnp.where(run >= gap, pltpu.roll(weight, shift, 0), 1.0)
    shift = 1 if down else RUNS - 1
    weight = jnp.where(run >= 1, pltpu.roll(weight, shift, 0), 1.0)
    return weight, jnp.where(run >= 1, pltpu.roll(value, shift, 0), 0.0)


def arrived(like, sem):
    pltpu.make_async_copy(like, like, sem).wait()


def told(sem, times):
    @pl.when(times > 0)
    def _():
        pl.semaphore_wait(sem, times)


def states_kernel(
    sizes,
    fade_hbm,
    update_hbm,
    gain_hbm,
    states,
    power_ref,
    fade,
    update,
    gain,
    flows,
    own,
    through,
    pieces,
    runs,
    message,
    inbox,
    powers,
    sent_sem,
    inbox_sem,
    power_sem,
    come_sem,
    near_sem,
    middle_sem,
    far_sem,
):
    n_time, n_chan = sizes
    groups, rows, _ = fade.shape
    length = rows * n_time
    steps = rows // (RUNS * PIECES)
    def places():
        me_t, me_c = lax.axis_index("time"), lax.axis_index("chan")
        row, cx = me_c // CHAN_RING, me_c % CHAN_RING
        around = [
            row * CHAN_RING + (cx + 1) % CHAN_RING,
            row * CHAN_RING + (cx + CHAN_RING - 1) % CHAN_RING,
            me_c + CHAN_RING - 2 * CHAN_RING * row,
        ]
        plane = me_t // PLANE
        lower_around = sum(jnp.where(peer < me_c, 1, 0) for peer in around)
        return me_t, me_c, plane, around, lower_around

    barrier = pltpu.get_barrier_semaphore()

    def spread(g):
        summed = None
        for i in [run * (rows // RUNS) + p for p in range(0, rows // RUNS, 16) for run in range(RUNS)]:
            at = pl.ds(i, 16)
            rate = fade[g, at]
            keep = jnp.exp2(rate * (-LOG2E / length))
            part = rate[:8] + rate[8:]
            summed = part if summed is None else summed + part
            push = update[g, at].astype(F32)
            for q in range(2):
                run, place = divmod(i + 8 * q, rows // RUNS)
                piece, step = divmod(place, steps)
                to = pl.ds(step * PITCH + run, 8, stride=PITCH)
                to_push = pl.ds(step * PITCH + RUNS + run, 8, stride=PITCH)
                flows[g * PIECES + piece, to] = keep[8 * q : 8 * q + 8]
                flows[g * PIECES + piece, to_push] = push[8 * q : 8 * q + 8]
        whole = jnp.exp2(jnp.sum(summed, axis=0, keepdims=True) * (-LOG2E / length))
        message[0, 0, g : g + 1] = whole
        message[1, 0, g : g + 1] = whole

    def backward_part(g):
        slabs = range(g * PIECES, (g + 1) * PIECES)
        weights = [flows[slab, pl.ds(0, RUNS)] for slab in slabs]
        behinds = [flows[slab, pl.ds(RUNS, RUNS)] for slab in slabs]
        for step in range(1, steps):
            at, at_push = pl.ds(step * PITCH, RUNS), pl.ds(step * PITCH + RUNS, RUNS)
            for p, slab in enumerate(slabs):
                behinds[p] = behinds[p] + weights[p] * flows[slab, at_push]
                weights[p] = weights[p] * flows[slab, at]
        for p, slab in enumerate(slabs):
            pieces[slab, 0], pieces[slab, 2] = weights[p], behinds[p]
        parts = list(zip(weights, behinds))
        while len(parts) > 1:
            parts = [
                (w0 * w1, b0 + w0 * b1) for (w0, b0), (w1, b1) in zip(parts[::2], parts[1::2])
            ]
        weight, behind = parts[0]
        runs[g, 0], runs[g, 2] = weight, behind
        for gap in (1, 2, 4):
            behind = behind + weight * pltpu.roll(behind, RUNS - gap, 0)
            weight = weight * pltpu.roll(weight, RUNS - gap, 0)
        message[1, 1, g : g + 1] = behind[:1]

    def forward_part(g):
        slabs = range(g * PIECES, (g + 1) * PIECES)
        aheads = [flows[slab, pl.ds(RUNS, RUNS)] for slab in slabs]
        for step in range(1, steps):
            at, at_push = pl.ds(step * PITCH, RUNS), pl.ds(step * PITCH + RUNS, RUNS)
            for p, slab in enumerate(slabs):
                aheads[p] = flows[slab, at] * aheads[p] + flows[slab, at_push]
        ahead = aheads[0]
        pieces[g * PIECES, 1] = ahead
        for p in range(1, PIECES):
            pieces[g * PIECES + p, 1] = aheads[p]
            ahead = aheads[p] + pieces[g * PIECES + p, 0] * ahead
        weight = runs[g, 0]
        runs[g, 1] = ahead
        for gap in (1, 2, 4):
            weight_next = pltpu.roll(weight, RUNS - gap, 0)
            ahead = pltpu.roll(ahead, RUNS - gap, 0) + weight_next * ahead
            weight = weight * weight_next
        message[0, 1, g : g + 1] = ahead[:1]

    def send_summary(me_t, me_c, k, way):
        pltpu.make_async_remote_copy(
            src_ref=message.at[way],
            dst_ref=inbox.at[me_t],
            send_sem=sent_sem,
            recv_sem=inbox_sem.at[way],
            device_id=(k, me_c),
            device_id_type=MESH,
        ).start()

    def load_and_send(load_sem, gain_sem):
        for g in range(groups):
            at = pl.ds(g * LANES, LANES)
            pltpu.make_async_copy(fade_hbm.at[0, :, at], fade.at[g], load_sem.at[g]).start()
            pltpu.make_async_copy(update_hbm.at[0, :, at], update.at[g], load_sem.at[g]).start()
        gain_load = pltpu.make_async_copy(gain_hbm, gain, gain_sem)
        gain_load.start()
        pl.delay(1)
        me_t, me_c, plane, around, lower_around = places()

        for peer in around:

            @pl.when(peer > me_c)
            def _():
                pl.semaphore_signal(barrier, inc=1, device_id=(me_t, peer), device_id_type=MESH)

        @pl.loop(me_t + 1, n_time)
        def _(k):
            pl.semaphore_signal(barrier, inc=1, device_id=(k, me_c), device_id_type=MESH)

        for g in range(groups + 1):
            if g < groups:
                arrived(fade.at[pl.ds(0, 3), pl.ds(0, rows // 2)], load_sem.at[g])
                spread(g)
            if g > 0:
                backward_part(g - 1)

        told(barrier, me_t + lower_around)

        @pl.loop(0, me_t)
        def _(k):
            send_summary(me_t, me_c, k, 1)

        for peer in around:

            @pl.when(peer < me_c)
            def _():
                pl.semaphore_signal(near_sem, inc=1, device_id=(me_t, peer), device_id_type=MESH)

        @pl.loop(0, me_t)
        def _(k):
            come = come_sem.at[plane]
            pl.semaphore_signal(come, inc=1, device_id=(k, me_c), device_id_type=MESH)

        gain_load.wait()

    pl.run_scoped(load_and_send, pltpu.SemaphoreType.DMA((groups,)), pltpu.SemaphoreType.DMA)

    me_t, me_c, plane, around, lower_around = places()

    for g in range(groups):
        forward_part(g)
    inbox[me_t] = message[0]

    told(come_sem.at[plane], PLANE - 1 - me_t % PLANE)

    @pl.loop(me_t + 1, (plane + 1) * PLANE)
    def _(k):
        send_summary(me_t, me_c, k, 0)

    def send_plane(to):
        @pl.when(to > plane)
        def _():
            pl.semaphore_wait(come_sem.at[to], PLANE)
            for k in range(to * PLANE, (to + 1) * PLANE):
                send_summary(me_t, me_c, k, 0)

    def tell_around(sem):
        for peer in around:
            pl.semaphore_signal(sem, inc=1, device_id=(me_t, peer), device_id_type=MESH)

    @pl.loop(0, groups)
    def _(g):
        slabs = [g * PIECES + p for p in range(PIECES)]
        down_in, ahead_in = scan_runs(runs[g, 0], runs[g, 1], True)
        up_in, behind_in = scan_runs(runs[g, 0], runs[g, 2], False)
        down, ahead, up, behind = [], [], [], []
        for slab in slabs:
            down.append(down_in)
            ahead.append(ahead_in)
            down_in = down_in * pieces[slab, 0]
            ahead_in = ahead_in * pieces[slab, 0] + pieces[slab, 1]
        for slab in slabs[::-1]:
            up.insert(0, up_in)
            behind.insert(0, behind_in)
            up_in = up_in * pieces[slab, 0]
            behind_in = behind_in * pieces[slab, 0] + pieces[slab, 2]
        for step in range(steps):
            at, at_2 = pl.ds(step * PITCH, RUNS), pl.ds(step * PITCH + RUNS, RUNS)
            for p, slab in enumerate(slabs):
                keep = flows[slab, at]
                ahead[p] = keep * ahead[p] + flows[slab, at_2]
                down[p] = keep * down[p]
                own[slab, at] = ahead[p]
                through[slab, at] = down[p]
        for step in range(steps - 1, -1, -1):
            at, at_2 = pl.ds(step * PITCH, RUNS), pl.ds(step * PITCH + RUNS, RUNS)
            for p, slab in enumerate(slabs):
                keep = flows[slab, at]
                behind[p] = keep * behind[p] + flows[slab, at_2]
                up[p] = keep * up[p]
                own[slab, at] = own[slab, at] + behind[p]
                own[slab, at_2] = up[p]

    told(near_sem, len(around) - lower_around)
    tell_around(middle_sem)
    for to in range(1, n_time // PLANE):
        send_plane(to)
    pl.semaphore_wait(middle_sem, len(around))
    tell_around(far_sem)

    def taken(k, state):
        return state * inbox[k, 0] + inbox[k, 1]

    for k in range(1, n_time):

        @pl.when(me_t == k)
        def _():
            arrived(inbox.at[pl.ds(0, k)], inbox_sem.at[0])

    zero = jnp.zeros((groups, LANES), F32)
    earlier = lax.fori_loop(0, me_t, taken, zero)
    for g in range(groups):
        entering = jnp.broadcast_to(earlier[g : g + 1], (RUNS, LANES))
        for slab in range(g * PIECES, (g + 1) * PIECES):
            for step in range(steps):
                at = pl.ds(step * PITCH, RUNS)
                own[slab, at] = own[slab, at] + through[slab, at] * entering

    for k in range(1, n_time):

        @pl.when(me_t == n_time - 1 - k)
        def _():
            arrived(inbox.at[pl.ds(0, k)], inbox_sem.at[1])

    joined = [
        (jnp.where(k > me_t, inbox[k, 0], 1.0), jnp.where(k > me_t, inbox[k, 1], 0.0))
        for k in range(n_time - 1, 0, -1)
    ]
    while len(joined) > 1:
        joined = [
            (joined[k][0] * joined[k + 1][0], joined[k][1] * joined[k + 1][0] + joined[k + 1][1])
            for k in range(0, len(joined) - 1, 2)
        ] + joined[len(joined) // 2 * 2 :]
    later = joined[0][1]

    entering = [jnp.broadcast_to(later[g : g + 1], (RUNS, LANES)) for g in range(groups)]

    def state_tile(g, row):
        run, place = divmod(row, rows // RUNS)
        piece, step = divmod(place, steps)
        slab, start = g * PIECES + piece, step * PITCH + run
        near = own[slab, pl.ds(start + RUNS, 8, stride=PITCH)]
        return own[slab, pl.ds(start, 8, stride=PITCH)] + near * entering[g]

    for b in range(rows // LANES):
        squares = []
        for row in range(b * LANES, (b + 1) * LANES, 8):
            total = None
            for g in range(groups):
                state = state_tile(g, row)
                square = state * state
                total = square if total is None else total + square
            squares.append(total)
        powers[me_c, b : b + 1] = jnp.sum(jnp.concatenate(squares, axis=0).T, axis=0, keepdims=True)

    pl.semaphore_wait(far_sem, len(around))
    for k in range(n_chan - 1):
        pltpu.make_async_remote_copy(
            src_ref=powers.at[me_c],
            dst_ref=powers.at[me_c],
            send_sem=sent_sem,
            recv_sem=power_sem,
            device_id=(me_t, k + jnp.where(k >= me_c, 1, 0)),
            device_id_type=MESH,
        ).start()
    for g in range(groups):
        gains = jnp.broadcast_to(gain[:, g * LANES : (g + 1) * LANES], (RUNS, LANES))
        for row in range(0, rows, 8):
            states[g, pl.ds(row, 8)] = state_tile(g, row) * gains
    arrived(powers.at[pl.ds(0, n_chan - 1)], power_sem)
    power = powers[0]
    for k in range(1, n_chan):
        power = power + powers[k]
    power_ref[...] = power

    sent = 2 * groups * (n_time - 1) + rows // LANES * (n_chan - 1)
    arrived(fade.at[0, pl.ds(0, sent)], sent_sem)


def norm_kernel(sizes, states, power, out_hbm, out, out_sem):
    channels, length = sizes
    groups, rows, _ = states.shape
    scale = lax.rsqrt(power[...] * (1.0 / channels) + 1e-06 * length)
    for b in range(rows // LANES):
        by_row = jnp.broadcast_to(scale[b : b + 1], (LANES, LANES)).T
        for h in range(2):
            part = pl.ds(b * LANES + h * (LANES // 2), LANES // 2)
            for g in range(groups):
                at = pl.ds(g * LANES, LANES)
                half = by_row[h * (LANES // 2) : (h + 1) * (LANES // 2)]
                out[part, at] = (states[g, part] * half).astype(BF16)
            pltpu.make_async_copy(out.at[part], out_hbm.at[0, part], out_sem).start()
    arrived(out, out_sem)


def per_device(fade_rate, update_in, norm_gain):
    n_time, n_chan = lax.axis_size("time"), lax.axis_size("chan")
    _, rows, columns = fade_rate.shape
    groups = columns // LANES
    anywhere = pl.BlockSpec(memory_space=pl.ANY)
    vmem = pl.BlockSpec(memory_space=pltpu.VMEM)
    slabs = pltpu.VMEM((PIECES * groups, rows // (PIECES * RUNS) * PITCH + 32, LANES), F32)
    states, power = pl.pallas_call(
        functools.partial(states_kernel, (n_time, n_chan)),
        out_shape=(
            pltpu.VMEM((groups, rows, LANES), F32),
            pltpu.VMEM((rows // LANES, LANES), F32),
        ),
        in_specs=[anywhere, anywhere, anywhere],
        out_specs=(vmem, vmem),
        scratch_shapes=[
            pltpu.VMEM((groups, rows, LANES), F32),
            pltpu.VMEM((groups, rows, LANES), BF16),
            pltpu.VMEM((1, columns), F32),
            slabs,
            slabs,
            slabs,
            pltpu.VMEM((PIECES * groups, 3, RUNS, LANES), F32),
            pltpu.VMEM((groups, 3, RUNS, LANES), F32),
            pltpu.VMEM((2, 2, groups, LANES), F32),
            pltpu.VMEM((n_time, 2, groups, LANES), F32),
            pltpu.VMEM((n_chan, rows // LANES, LANES), F32),
            pltpu.SemaphoreType.DMA,
            pltpu.SemaphoreType.DMA((2,)),
            pltpu.SemaphoreType.DMA,
            pltpu.SemaphoreType.REGULAR((n_time // PLANE,)),
            pltpu.SemaphoreType.REGULAR,
            pltpu.SemaphoreType.REGULAR,
            pltpu.SemaphoreType.REGULAR,
        ],
        compiler_params=pltpu.CompilerParams(collective_id=0, has_side_effects=True),
        name="filter_states",
    )(fade_rate, update_in, norm_gain.reshape(1, columns))
    states, power = (pltpu.with_memory_space_constraint(x, pltpu.VMEM) for x in (states, power))
    return pl.pallas_call(
        functools.partial(norm_kernel, (columns * n_chan, rows * n_time)),
        out_shape=jax.ShapeDtypeStruct((1, rows, columns), BF16),
        in_specs=[vmem, vmem],
        out_specs=anywhere,
        scratch_shapes=[
            pltpu.VMEM((rows, columns), BF16),
            pltpu.SemaphoreType.DMA,
        ],
        name="channel_norm",
    )(states, power)


def solution(mesh):
    return jax.shard_map(
        per_device,
        mesh=mesh,
        in_specs=(P(None, "time", "chan"), P(None, "time", "chan"), P("chan")),
        out_specs=P(None, "time", "chan"),
        check_vma=False,
    )
```
